128 devices in a mesh: section: 4 (over y), fsdp: 32 (over x, z, core).
Axes of the slice: x: 4, y: 4, z: 4, core: 2. Of those that a mesh axis runs over, the one named last changes fastest.
Arguments:
- patches: bfloat16 [8, 4096, 768], P(None, 'fsdp'), may hold values from -6 to 6
- cotangent: bfloat16 [8, 4096, 768], P(None, 'fsdp'), may hold values from -6 to 6
- embed_blocks: int32 [8], replicated, may hold values from 4 to 6
- ratio_index: int32 [8], replicated, may hold values from 0 to 2
- depth: int32 [8], replicated, may hold values from 2 to 4
- w_up: bfloat16 [4, 768, 3072], P('section', 'fsdp'), may hold values from -0.21875 to 0.21875
- w_down: bfloat16 [4, 3072, 768], P('section', 'fsdp'), may hold values from -0.109375 to 0.109375
- ln_gain: bfloat16 [4, 768], P('section', 'fsdp'), may hold values from 0.099609375 to 1.8984375
Outputs:
- grad_up: float32 [4, 768, 3072], P('section', 'fsdp')
- grad_down: float32 [4, 3072, 768], P('section', 'fsdp')
- grad_gain: float32 [4, 768], P('section', 'fsdp')
The draws below stay inside these ranges and needn't reach their ends.
All inputs are finite; a program needn't handle non-finite values.
Results may differ from the reference program's by a relative error of at most 0.028.
Values may be sent and summed in bfloat16 or wider, within the bound.
No kernel may reach another device: no remote copies, remote signals or barrier semaphores. Data moves between devices by JAX's collectives and lax.ppermute only.
A program may use at most 192 MiB of HBM per device.

```python
import jax
import jax.numpy as jnp
from jax import lax

D = 768
FF = 3072
BLOCK = 128
MICRO = 8
LAYERS = 4
TOKENS = 4096
N_SECTION = 4


def plant(values, stream_key, low, top_value):
    longest = values.shape.index(max(values.shape))
    spots = []
    for shift in (0, 1):
        where = [jax.random.randint(jax.random.fold_in(stream_key, axis), (), 0, length) for axis, length in enumerate(values.shape)]
        where[longest] = (where[longest] + shift) % values.shape[longest]
        spots.append(tuple(where))
    return values.at[spots[0]].set(low).at[spots[1]].set(top_value)


def strengthened(entries, own_key, source, target, blocks, factor):
    def block_of(position):
        return (jnp.arange(entries.shape[position]) // (entries.shape[position] // blocks)).reshape((-1,) + (1,) * (entries.ndim - 1 - position))

    first = jax.random.permutation(own_key, blocks)[block_of(target)]
    far = (block_of(target) + blocks // 2) % blocks
    return jnp.where((block_of(source) == first) | (block_of(source) == far), factor * entries, entries)


def level_of(stream_key, dims, split, least, high):
    gain = 1.0
    for axis_at, parts in split:
        steps = jax.random.uniform(jax.random.fold_in(jax.random.fold_in(stream_key, 6), axis_at), (parts,), jnp.float32, least / len(split), high / len(split))
        gain = gain * jnp.repeat(jnp.exp(steps), dims[axis_at] // parts).reshape((-1,) + (1,) * (len(dims) - 1 - axis_at))
    return gain


def scatter_about(rng, extent, spread, limit, cuts=(), dtype=jnp.bfloat16):
    values = jax.random.normal(rng, extent, jnp.float32) * spread
    if len(cuts) > 0:
        values = level_of(rng, extent, cuts, -0.22, 0.18) * values
    return jnp.clip(values, min=-limit, max=limit).astype(dtype)


def bell_draw_with(rng, shape, scale, bound, shards, heavy, dtype=jnp.bfloat16):
    entries = scale * jax.random.normal(rng, shape, jnp.float32)
    if shards:
        entries = entries * level_of(rng, shape, shards, -0.22, 0.18)
    return jnp.clip(strengthened(entries, jax.random.fold_in(rng, 3), *heavy), -bound, bound).astype(dtype)


def setup_inputs(seed: int = 0) -> dict:
    seeds = jax.random.split(jax.random.key(seed), 9)
    return {
        "patches": scatter_about(seeds[0], (MICRO, TOKENS, D), 1.0, 6.0, ((1, 32),)),
        "cotangent": bell_draw_with(seeds[1], (MICRO, TOKENS, D), 1.0, 6.0, ((1, 32),), (1, 2, 32, 2.75)),
        "embed_blocks": plant(jax.random.randint(seeds[2], (MICRO,), D // BLOCK - 2, D // BLOCK + 1), jax.random.fold_in(seeds[2], 1), D // BLOCK - 2, (D // BLOCK + 1) - 1).astype(jnp.int32),
        "ratio_index": plant(jax.random.randint(seeds[3], (MICRO,), 0, 3), jax.random.fold_in(seeds[3], 1), 0, 2).astype(jnp.int32),
        "depth": plant(jax.random.randint(seeds[4], (MICRO,), N_SECTION - 2, N_SECTION + 1), jax.random.fold_in(seeds[4], 1), N_SECTION - 2, N_SECTION).astype(jnp.int32),
        "w_up": scatter_about(seeds[5], (LAYERS, D, FF), D ** -0.5, 0.21875, ((0, 4), (1, 32))),
        "w_down": scatter_about(seeds[6], (LAYERS, FF, D), FF ** -0.5, 0.109375, ((0, 4), (1, 32))),
        "ln_gain": jnp.clip(1.0 + 0.18 * jax.random.normal(seeds[7], (LAYERS, D), jnp.float32), 0.099609375, 1.8984375).astype(jnp.bfloat16),
    }


EPSILON = 1e-05

def micro_masks(blocks, ratio, feature_count, hidden_count):
    width_int = (blocks * BLOCK).astype(jnp.int32)
    hidden_int = (width_int * (6 + ratio) // 2).astype(jnp.int32)
    embed_mask = (lax.iota(jnp.int32, feature_count) < width_int).astype(jnp.float32)
    hidden_mask = (lax.iota(jnp.int32, hidden_count) < hidden_int).astype(jnp.float32)
    return (embed_mask, hidden_mask, width_int.astype(jnp.float32))

def layer_norm(inputs, embed_mask, width_float):
    values = inputs.astype(jnp.float32) * embed_mask
    center_value = lax.optimization_barrier(jnp.sum(values, axis=-1, keepdims=True)) / width_float
    centered = (values - center_value) * embed_mask
    variance = lax.optimization_barrier(jnp.sum(centered * centered, axis=-1, keepdims=True)) / width_float
    inv_std = lax.rsqrt(variance + EPSILON)
    return (centered * inv_std, inv_std)

def layer_forward(inputs, gain_vector, weight_up, weight_down, embed_mask, hidden_mask, active, width_float):
    standard, inv_std = layer_norm(inputs, embed_mask, width_float)
    normed = (standard * gain_vector.astype(jnp.float32)).astype(jnp.bfloat16)
    hidden = jnp.dot(normed, weight_up, preferred_element_type=jnp.float32)
    activated = (jax.nn.gelu(hidden) * hidden_mask).astype(jnp.bfloat16)
    branch = jnp.dot(activated, weight_down, preferred_element_type=jnp.float32)
    output = (inputs.astype(jnp.float32) + active * embed_mask * branch).astype(jnp.bfloat16)
    return (output, hidden)

def layer_backward(inputs, hidden, grad_out, gain_vector, weight_up, weight_down, embed_mask, hidden_mask, active, width_float):
    standard, inv_std = layer_norm(inputs, embed_mask, width_float)
    gain_float = gain_vector.astype(jnp.float32)
    normed = (standard * gain_float).astype(jnp.bfloat16)
    activated = (jax.nn.gelu(hidden) * hidden_mask).astype(jnp.bfloat16)
    grad_branch = (active * embed_mask * grad_out.astype(jnp.float32)).astype(jnp.bfloat16)
    grad_act = lax.dot_general(grad_branch, weight_down, (((1,), (1,)), ((), ())), preferred_element_type=jnp.float32)
    unused, pullback = jax.vjp(jax.nn.gelu, hidden)
    grad_hidden = pullback(grad_act * hidden_mask)[0].astype(jnp.bfloat16)
    grad_normed = lax.dot_general(grad_hidden, weight_up, (((1,), (1,)), ((), ())), preferred_element_type=jnp.float32)
    grad_standard = grad_normed * gain_float * embed_mask
    grad_gain = lax.optimization_barrier(jnp.sum(grad_normed * standard, axis=0))
    first_mean = lax.optimization_barrier(jnp.sum(grad_standard, axis=-1, keepdims=True)) / width_float
    second_mean = lax.optimization_barrier(jnp.sum(grad_standard * standard, axis=-1, keepdims=True)) / width_float
    grad_norm_in = inv_std * (grad_standard - first_mean * embed_mask - standard * second_mean)
    grad_in = (grad_out.astype(jnp.float32) + grad_norm_in).astype(jnp.bfloat16)
    return (grad_in, normed, grad_hidden, activated, grad_branch, grad_gain)

def contract_rows(left, right):
    return lax.dot_general(left, right, (((0,), (0,)), ((), ())), preferred_element_type=jnp.float32)

def reference(patches, cotangent, embed_blocks, ratio_index, depth, w_up, w_down, ln_gain):
    feature_count = w_up.shape[1]
    hidden_count = w_up.shape[2]
    grads_up = [jnp.zeros((feature_count, hidden_count), jnp.float32) for layer_number in range(LAYERS)]
    grads_down = [jnp.zeros((hidden_count, feature_count), jnp.float32) for layer_number in range(LAYERS)]
    grads_gain = [jnp.zeros((feature_count,), jnp.float32) for layer_number in range(LAYERS)]
    for micro_number in range(MICRO):
        embed_mask, hidden_mask, width_float = micro_masks(embed_blocks[micro_number], ratio_index[micro_number], feature_count, hidden_count)
        inputs = (patches[micro_number].astype(jnp.float32) * embed_mask).astype(jnp.bfloat16)
        saved = []
        for layer_number in range(LAYERS):
            active = (layer_number < depth[micro_number]).astype(jnp.float32)
            output, hidden = layer_forward(inputs, ln_gain[layer_number], w_up[layer_number], w_down[layer_number], embed_mask, hidden_mask, active, width_float)
            saved.append((inputs, hidden, active))
            inputs = output
        grad_out = (cotangent[micro_number].astype(jnp.float32) * embed_mask).astype(jnp.bfloat16)
        for layer_number in reversed(range(LAYERS)):
            layer_in, hidden, active = saved[layer_number]
            grad_in, normed, grad_hidden, activated, grad_branch, grad_gain = layer_backward(layer_in, hidden, grad_out, ln_gain[layer_number], w_up[layer_number], w_down[layer_number], embed_mask, hidden_mask, active, width_float)
            grads_up[layer_number] = grads_up[layer_number] + contract_rows(normed, grad_hidden)
            grads_down[layer_number] = grads_down[layer_number] + contract_rows(activated, grad_branch)
            grads_gain[layer_number] = grads_gain[layer_number] + grad_gain
            grad_out = grad_in
    return (jnp.stack(grads_up), jnp.stack(grads_down), jnp.stack(grads_gain))
```

```python
import functools

import jax
import jax.numpy as jnp
from jax import lax
from jax.experimental import pallas as pl
from jax.experimental.pallas import tpu as pltpu
from jax.sharding import Mesh
from jax.sharding import PartitionSpec as P

BLOCK = 128
EPSILON = 1e-05
AX, AZ, AC = "fsdp_0", "fsdp_1", "fsdp_2"
FSDP = (AX, AZ, AC)
SKEW = 2
CHUNK = 512
GELU_A = 0.7978845608028654
GELU_B = GELU_A * 0.044715
BF16, F32 = jnp.bfloat16, jnp.float32


ANY = pl.BlockSpec(memory_space=pl.ANY)
SMEM = pl.BlockSpec(memory_space=pltpu.SMEM)
VMEM = pl.BlockSpec(memory_space=pltpu.VMEM)


def shift(value, axis, distance, wrap=True):
    n = lax.axis_size(axis)
    if wrap:
        route = [(i, (i + distance) % n) for i in range(n)]
    else:
        route = [(i, i + distance) for i in range(n) if 0 <= i + distance < n]
    return lax.ppermute(value, axis, route)


def gather_pieces(own, first, second):
    line = jnp.stack([own] + [shift(own, first, -r) for r in (1, 2, 3)])
    ahead, behind = shift(line, second, -1), shift(line, second, 1)
    low = shift(behind[:2], second, 1)
    high = shift(ahead[2:], second, -1)
    mine = (line, ahead, behind, low, high)
    return mine + tuple(shift(p, AC, 1) for p in mine)


def placements(first_at, second_at, core):
    rows = []
    for own in (0, 1):
        c = core if own == 0 else 1 - core
        for piece, r2, r1s in ((0, 0, range(4)), (1, 1, range(4)), (2, 3, range(4)), (3, 2, (0, 1)), (4, 2, (2, 3))):
            for at, r1 in enumerate(r1s):
                rows.append((5 * own + piece, at, (first_at + r1) & 3, (second_at + r2) & 3, c))
    return rows


def assemble_kernel(place, *refs):
    ups, downs, (w_up, w_down), (up_buf, down_buf, sem_up, sem_down, sem_out) = refs[:10], refs[10:20], refs[20:22], refs[22:]
    x, z, c = place[0], place[1], place[2]
    n_chunk = w_up.shape[0]
    loads = []
    for piece, at, fx, fz, core in placements(x, z, c):
        loads.append(pltpu.make_async_copy(ups[piece].at[at], up_buf.at[fx * 8 + fz * 2 + core], sem_up.at[len(loads)]))
    late = []
    for piece, at, fz, fx, core in placements(z, x, c):
        late.append(pltpu.make_async_copy(downs[piece].at[at], down_buf.at[fx * 8 + fz * 2 + core], sem_down.at[len(late)]))
    for copy in loads + late:
        copy.start()
    for copy in loads:
        copy.wait()
    stores = [
        pltpu.make_async_copy(up_buf.at[:, :, k * CHUNK : (k + 1) * CHUNK], w_up.at[k], sem_out.at[k]) for k in range(n_chunk)
    ]
    for copy in stores:
        copy.start()
    for copy in late:
        copy.wait()
    stores.append(pltpu.make_async_copy(down_buf, w_down, sem_out.at[n_chunk]))
    stores[-1].start()
    for copy in stores:
        copy.wait()


def gather_weights(up, down, place):
    ups = gather_pieces(up, AX, AZ)
    downs = gather_pieces(down, AZ, AX)
    n_chunk = up.shape[1] // CHUNK
    w_up, w_down = pl.pallas_call(
        assemble_kernel,
        out_shape=(
            jax.ShapeDtypeStruct((n_chunk, 32, up.shape[0], CHUNK), BF16),
            jax.ShapeDtypeStruct((32,) + down.shape, BF16),
        ),
        in_specs=[SMEM] + [ANY] * 20,
        out_specs=(ANY, ANY),
        scratch_shapes=[
            pltpu.VMEM((32,) + up.shape, BF16),
            pltpu.VMEM((32,) + down.shape, BF16),
            pltpu.SemaphoreType.DMA((32,)),
            pltpu.SemaphoreType.DMA((32,)),
            pltpu.SemaphoreType.DMA((n_chunk + 1,)),
        ],
        name="assemble",
    )(place, *ups, *downs)
    return w_up.reshape(n_chunk, -1, CHUNK), w_down.reshape(n_chunk, CHUNK, -1)


def norm_of(values, mask, width):
    mean = jnp.sum(values, axis=-1, keepdims=True) / width
    centered = jnp.where(mask, values - mean, 0.0)
    variance = jnp.sum(centered * centered, axis=-1, keepdims=True) / width
    inv_std = lax.rsqrt(variance + EPSILON)
    return centered * inv_std, inv_std


def fetch(source, target, sem):
    copy = pltpu.make_async_copy(source, target, sem)
    copy.start()
    return copy


def forward_kernel(*refs, tick, has_input, aliased, micros):
    refs = list(refs)
    tab = refs.pop(0)
    if tick is None:
        tick = refs.pop(0)[0]
    patches = refs.pop(0)
    incoming = refs.pop(0) if has_input else None
    w_up, w_down = refs.pop(0), refs.pop(0)
    refs = refs[aliased:]
    out, x_st, st_st, at_st, gp_st = refs[:5]
    x_buf, st_buf, at_buf, gp_buf, up_buf, down_buf, acc, sem_x, sem_w, sem_out = refs[5:]
    n_chunk = up_buf.shape[0]
    sec = tab[4 * micros]
    q = tick - SKEW * sec
    at = jnp.clip(q, 0, micros - 1)
    micro, width, hidden, depth = tab[at], tab[micros + at], tab[2 * micros + at], tab[3 * micros + at]
    valid = jnp.logical_and(jnp.logical_and(q >= 0, q < micros), depth > sec)

    def up_copy(c):
        return pltpu.make_async_copy(w_up.at[c], up_buf.at[c], sem_w.at[2 * c])

    def down_copy(c):
        return pltpu.make_async_copy(w_down.at[c], down_buf.at[c], sem_w.at[2 * c + 1])

    @pl.when(valid)
    def run():
        used = (hidden + CHUNK - 1) // CHUNK
        if has_input:

            @pl.when(sec == 0)
            def first():
                fetch(patches.at[micro], x_buf, sem_x).wait()

            @pl.when(sec != 0)
            def later():
                fetch(incoming, x_buf, sem_x).wait()
        else:
            load = fetch(patches.at[micro], x_buf, sem_x)
        for c in range(n_chunk):

            @pl.when(c < used)
            def start(c=c):
                up_copy(c).start()
                down_copy(c).start()

        if not has_input:
            load.wait()
        mask = lax.broadcasted_iota(jnp.int32, x_buf.shape, 1) < width
        values = jnp.where(mask, x_buf[...].astype(F32), 0.0)
        x_buf[...] = values.astype(BF16)
        standard, _ = norm_of(values, mask, width.astype(F32))
        st_buf[...] = standard.T.astype(BF16)
        normed = standard.astype(BF16)
        copies = [fetch(x_buf, x_st.at[at], sem_out.at[0]), fetch(st_buf, st_st.at[at], sem_out.at[1])]
        acc[...] = values

        @pl.loop(0, used)
        def step(c):
            up_copy(c).wait()
            half = CHUNK // 2
            hids = [
                jnp.dot(normed, up_buf[c, :, j * half : (j + 1) * half], preferred_element_type=F32) for j in range(2)
            ]
            parts = []
            for j, h in enumerate(hids):
                h2 = h * h
                t = jnp.tanh(h * (GELU_A + GELU_B * h2))
                p = 0.5 + 0.5 * t
                act = h * p
                slope = p + act * (1.0 - t) * (GELU_A + (3.0 * GELU_B) * h2)
                unit = lax.broadcasted_iota(jnp.int32, h.shape, 1) + (c * CHUNK + j * half)
                inside = unit < hidden
                act = jnp.where(inside, act, 0.0)
                at_buf[c, j * half : (j + 1) * half, :] = act.T.astype(BF16)
                gp_buf[c, :, j * half : (j + 1) * half] = jnp.where(inside, slope, 0.0).astype(BF16)
                parts.append(act.astype(BF16))
            down_copy(c).wait()
            acc[...] += jnp.dot(jnp.concatenate(parts, 1), down_buf[c], preferred_element_type=F32)

        @pl.loop(used, n_chunk)
        def clear(c):
            at_buf[c] = jnp.zeros(at_buf.shape[1:], BF16)

        copies += [fetch(at_buf, at_st.at[at], sem_out.at[2]), fetch(gp_buf, gp_st.at[at], sem_out.at[3])]
        out[...] = jnp.where(mask, acc[...], 0.0).astype(BF16)
        for copy in copies:
            copy.wait()


def forward(tick, tab, patches, incoming, w_up, w_down, stash):
    micros, rows, feat = patches.shape
    n_chunk = w_up.shape[0]
    x_st, st_st, at_st, gp_st = stash
    slot = jax.ShapeDtypeStruct
    outs = (
        slot((rows, feat), BF16),
        slot((micros, rows, feat), BF16),
        slot((micros, feat, rows), BF16),
        slot((micros, n_chunk, CHUNK, rows), BF16),
        slot((micros, n_chunk, rows, CHUNK), BF16),
    )
    operands, specs = [tab], [SMEM]
    static = tick if isinstance(tick, int) else None
    if static is None:
        operands.append(tick.reshape(1))
        specs.append(SMEM)
    operands.append(patches)
    if incoming is not None:
        operands.append(incoming)
    operands += [w_up, w_down]
    alias = {}
    aliased = 0
    base = len(operands)
    for k, s in enumerate((x_st, st_st, at_st, gp_st)):
        if s is not None:
            alias[len(operands)] = k + 1
            operands.append(s)
            aliased += 1
    specs += [ANY] * (len(operands) - len(specs))
    body = functools.partial(
        forward_kernel, tick=static, has_input=incoming is not None, aliased=aliased, micros=micros
    )
    out, *stash = pl.pallas_call(
        body,
        out_shape=outs,
        in_specs=specs,
        out_specs=(VMEM, ANY, ANY, ANY, ANY),
        scratch_shapes=[
            pltpu.VMEM((rows, feat), BF16),
            pltpu.VMEM((feat, rows), BF16),
            pltpu.VMEM((n_chunk, CHUNK, rows), BF16),
            pltpu.VMEM((n_chunk, rows, CHUNK), BF16),
            pltpu.VMEM((n_chunk, feat, CHUNK), BF16),
            pltpu.VMEM((n_chunk, CHUNK, feat), BF16),
            pltpu.VMEM((rows, feat), F32),
            pltpu.SemaphoreType.DMA,
            pltpu.SemaphoreType.DMA((2 * n_chunk,)),
            pltpu.SemaphoreType.DMA((4,)),
        ],
        input_output_aliases=alias,
        name="forward",
    )(*operands)
    return out, tuple(stash)


def backward_kernel(*refs, tick, micros):
    refs = list(refs)
    tab = refs.pop(0)
    if tick is None:
        tick = refs.pop(0)[0]
    cotangent, incoming, w_up, w_down, x_st, gp_st = refs[:6]
    refs = refs[9:]
    out, g_st, gh_st, gg_st = refs[:4]
    x_buf, g_buf, gp_buf, gh_buf, gg_buf, up_buf, down_buf, acc, sem_g, sem_x, sem_w, sem_out = refs[4:]
    n_chunk = up_buf.shape[0]
    sec = tab[4 * micros]
    q = (micros - 1) - (tick + SKEW * (sec - 1))
    at = jnp.clip(q, 0, micros - 1)
    micro, width, hidden, depth = tab[at], tab[micros + at], tab[2 * micros + at], tab[3 * micros + at]
    valid = jnp.logical_and(jnp.logical_and(q >= 0, q < micros), depth > sec)

    def up_copy(c):
        return pltpu.make_async_copy(w_up.at[c], up_buf.at[c], sem_w.at[2 * c])

    def down_copy(c):
        return pltpu.make_async_copy(w_down.at[c], down_buf.at[c], sem_w.at[2 * c + 1])

    @pl.when(valid)
    def run():
        used = (hidden + CHUNK - 1) // CHUNK

        @pl.when(depth == sec + 1)
        def last():
            fetch(cotangent.at[micro], g_buf, sem_g).wait()

        @pl.when(depth != sec + 1)
        def inner():
            fetch(incoming, g_buf, sem_g).wait()

        loads = [fetch(gp_st.at[at], gp_buf, sem_x.at[0]), fetch(x_st.at[at], x_buf, sem_x.at[1])]
        for c in range(n_chunk):

            @pl.when(c < used)
            def start(c=c):
                down_copy(c).start()
                up_copy(c).start()

        mask = lax.broadcasted_iota(jnp.int32, x_buf.shape, 1) < width
        grad_out = jnp.where(mask, g_buf[...].astype(F32), 0.0)
        g_buf[...] = grad_out.astype(BF16)
        grad_branch = g_buf[...]
        copies = [fetch(g_buf, g_st.at[at], sem_out.at[0])]
        for load in loads:
            load.wait()
        acc[...] = jnp.zeros(acc.shape, F32)

        @pl.loop(0, used)
        def step(c):
            nt = (((1,), (1,)), ((), ()))
            down_copy(c).wait()
            grad_act = lax.dot_general(grad_branch, down_buf[c], nt, preferred_element_type=F32)
            grad_hid = (grad_act * gp_buf[c].astype(F32)).astype(BF16)
            gh_buf[c] = grad_hid
            up_copy(c).wait()
            acc[...] += lax.dot_general(grad_hid, up_buf[c], nt, preferred_element_type=F32)

        @pl.loop(used, n_chunk)
        def clear(c):
            gh_buf[c] = jnp.zeros(gh_buf.shape[1:], BF16)

        copies.append(fetch(gh_buf, gh_st.at[at], sem_out.at[1]))
        width_float = width.astype(F32)
        standard, inv_std = norm_of(x_buf[...].astype(F32), mask, width_float)
        grad_std = jnp.where(mask, acc[...], 0.0)
        product = grad_std * standard
        gg_buf[...] = jnp.sum(product.reshape(-1, 8, product.shape[1]), axis=0)
        copies.append(fetch(gg_buf, gg_st.at[at], sem_out.at[2]))
        first_mean = jnp.sum(grad_std, axis=-1, keepdims=True) / width_float
        second_mean = jnp.sum(product, axis=-1, keepdims=True) / width_float
        grad_in = inv_std * (grad_std - first_mean - standard * second_mean)
        out[...] = jnp.where(mask, grad_out + grad_in, 0.0).astype(BF16)
        for copy in copies:
            copy.wait()


def backward(tick, tab, cotangent, incoming, w_up, w_down, x_st, gp_st, stash):
    micros, rows, feat = cotangent.shape
    n_chunk = w_up.shape[0]
    slot = jax.ShapeDtypeStruct
    operands, specs = [tab], [SMEM]
    static = tick if isinstance(tick, int) else None
    if static is None:
        operands.append(tick.reshape(1))
        specs.append(SMEM)
    operands += [cotangent, incoming, w_up, w_down, x_st, gp_st]
    alias = {len(operands) + k: k + 1 for k in range(3)}
    operands += list(stash)
    specs += [ANY] * (len(operands) - len(specs))
    out, *stash = pl.pallas_call(
        functools.partial(backward_kernel, tick=static, micros=micros),
        out_shape=(
            slot((rows, feat), BF16),
            slot((micros, rows, feat), BF16),
            slot((micros, n_chunk, rows, CHUNK), BF16),
            slot((micros, 8, feat), F32),
        ),
        in_specs=specs,
        out_specs=(VMEM, ANY, ANY, ANY),
        scratch_shapes=[
            pltpu.VMEM((rows, feat), BF16),
            pltpu.VMEM((rows, feat), BF16),
            pltpu.VMEM((n_chunk, rows, CHUNK), BF16),
            pltpu.VMEM((n_chunk, rows, CHUNK), BF16),
            pltpu.VMEM((8, feat), F32),
            pltpu.VMEM((n_chunk, feat, CHUNK), BF16),
            pltpu.VMEM((n_chunk, CHUNK, feat), BF16),
            pltpu.VMEM((rows, feat), F32),
            pltpu.SemaphoreType.DMA,
            pltpu.SemaphoreType.DMA((2,)),
            pltpu.SemaphoreType.DMA((2 * n_chunk,)),
            pltpu.SemaphoreType.DMA((3,)),
        ],
        input_output_aliases=alias,
        name="backward",
    )(*operands)
    return out, tuple(stash)


def split_cores(core, blocks, mine, theirs, value_of):
    for parity, targets in ((0, (mine, theirs)), (1, (theirs, mine))):

        @pl.when(core == parity)
        def write(targets=targets):
            for f in range(blocks):
                targets[f & 1](f >> 3, (f >> 1) & 3, value_of(f))


def up_kernel(place, st, gh, gg, up_own, up_par, gain_own, gain_par):
    x, z, core = place[0], place[1], place[2]
    micros = st.shape[0]

    def put(ref):
        def write(fx, fz, value):
            ref[(fx - x) & 3, (fz - z) & 3] = value

        return write

    left = jnp.concatenate([st[i] for i in range(micros)], axis=1)
    right = jnp.concatenate([gh[i, 0] for i in range(micros)], axis=0)
    up = jnp.dot(left, right, preferred_element_type=F32).astype(BF16)
    n = up.shape[0] // 32
    split_cores(core, 32, put(up_own), put(up_par), lambda f: up[f * n : (f + 1) * n])

    @pl.when(pl.program_id(0) == 0)
    def gains():
        total = gg[...].reshape(-1, gg.shape[2])
        total = jnp.concatenate([total, jnp.zeros((128 - total.shape[0], total.shape[1]), F32)], axis=0)
        column = total.T.astype(BF16)
        split_cores(core, 32, put(gain_own), put(gain_par), lambda f: column[f * n : (f + 1) * n])


def up_grads(place, st_st, gh_st, gg_st):
    micros, feat, rows = st_st.shape
    n_chunk = gh_st.shape[1]
    part = feat // 32
    wide = jax.ShapeDtypeStruct((4, 4, part, n_chunk * CHUNK), BF16)
    thin = jax.ShapeDtypeStruct((4, 4, part, 128), BF16)
    wide_spec = pl.BlockSpec((4, 4, part, CHUNK), lambda c: (0, 0, 0, c))
    thin_spec = pl.BlockSpec((4, 4, part, 128), lambda c: (0, 0, 0, 0))
    return pl.pallas_call(
        up_kernel,
        grid=(n_chunk,),
        out_shape=(wide, wide, thin, thin),
        in_specs=[
            SMEM,
            pl.BlockSpec((micros, feat, rows), lambda c: (0, 0, 0)),
            pl.BlockSpec((micros, 1, rows, CHUNK), lambda c: (0, c, 0, 0)),
            pl.BlockSpec(gg_st.shape, lambda c: (0, 0, 0)),
        ],
        out_specs=(wide_spec, wide_spec, thin_spec, thin_spec),
        name="up_grads",
    )(place, st_st, gh_st, gg_st)


def down_kernel(place, at, g, own, par):
    core, z = place[2], place[1]
    micros = at.shape[0]
    right = g[...].reshape(-1, g.shape[2])
    left = jnp.concatenate([at[i].reshape(-1, at.shape[3]) for i in range(micros)], axis=1)
    down = jnp.dot(left, right, preferred_element_type=F32).astype(BF16)
    n = down.shape[0] // 8
    for parity, targets in ((0, (own, par)), (1, (par, own))):

        @pl.when(core == parity)
        def write(targets=targets):
            for f in range(8):
                targets[f & 1][((f >> 1) - z) & 3, 0] = down[f * n : (f + 1) * n]


def down_grads(place, at_st, g_st):
    micros, n_chunk, _, rows = at_st.shape
    feat = g_st.shape[2]
    wide = n_chunk * CHUNK // 4
    unit = 256
    at_view = at_st.reshape(micros, n_chunk * CHUNK // unit, unit, rows)
    part = n_chunk * CHUNK // 32
    out = jax.ShapeDtypeStruct((4, 4, part, feat), BF16)
    spec = pl.BlockSpec((4, 1, part, feat), lambda i, p: (0, (i - p[0]) & 3, 0, 0))
    return pl.pallas_call(
        down_kernel,
        grid_spec=pltpu.PrefetchScalarGridSpec(
            num_scalar_prefetch=1,
            grid=(4,),
            in_specs=[
                pl.BlockSpec((micros, wide // unit, unit, rows), lambda i, p: (0, i, 0, 0)),
                pl.BlockSpec(g_st.shape, lambda i, p: (0, 0, 0)),
            ],
            out_specs=(spec, spec),
        ),
        out_shape=(out, out),
        name="down_grads",
    )(place, at_view, g_st)


def plus(*values):
    total = values[0].astype(F32)
    for v in values[1:]:
        total = total + v.astype(F32)
    return total


def scatter_sum(own, partner, first, second):
    other = shift(partner, AC, 1)

    def joined(*at):
        return plus(own[at], other[at])

    low = shift(joined(2, slice(0, 2)).astype(BF16), first, 1)
    high = shift(joined(2, slice(2, 4)).astype(BF16), first, -1)
    ahead = jnp.concatenate([plus(joined(1, slice(0, 2)), low), joined(1, slice(2, 4))]).astype(BF16)
    behind = jnp.concatenate([joined(3, slice(0, 2)), plus(joined(3, slice(2, 4)), high)]).astype(BF16)
    line = plus(joined(0), shift(ahead, first, 1), shift(behind, first, -1))
    parts = [shift(line[r].astype(BF16), second, r) for r in (1, 2, 3)]
    return plus(line[0], *parts)


def schedule_table(embed_blocks, ratio_index, depth):
    micros = depth.shape[0]
    index = lax.iota(jnp.int32, micros)
    before = jnp.logical_or(
        depth[None, :] > depth[:, None],
        jnp.logical_and(depth[None, :] == depth[:, None], index[None, :] < index[:, None]),
    )
    rank = jnp.sum(before.astype(jnp.int32), axis=1)
    chosen = rank[None, :] == index[:, None]
    width = embed_blocks * BLOCK
    hidden = width * (6 + ratio_index) // 2
    columns = jnp.stack([index, width, hidden, depth])
    table = jnp.sum(jnp.where(chosen[None], columns[:, None, :], 0), axis=2)
    section = lax.axis_index("section").astype(jnp.int32)
    return jnp.concatenate([table.reshape(-1), jnp.full((8,), section, jnp.int32)])


def per_device(patches, cotangent, embed_blocks, ratio_index, depth, w_up, w_down, ln_gain):
    sections = lax.axis_size("section")
    micros, rows, feat = patches.shape
    hidden = w_up.shape[2]
    n_chunk = hidden // CHUNK
    gain = ln_gain[0].astype(F32)[:, None]
    place = jnp.stack([lax.axis_index(a) for a in FSDP]).astype(jnp.int32)
    tab = schedule_table(embed_blocks, ratio_index, depth)
    scaled = (w_up[0].astype(F32) * gain).astype(BF16)
    up, down = gather_weights(scaled, w_down[0], place)

    reach = [jnp.sum((depth > s).astype(jnp.int32)) for s in range(sections)]
    main = micros + SKEW
    ticks = functools.reduce(jnp.maximum, [n + SKEW * s for s, n in enumerate(reach) if s > 1], main)
    lead = functools.reduce(
        jnp.maximum, [n + SKEW * (s - 1) for s, n in enumerate(reach) if s > 1], micros
    ) - micros

    stash = (None, jnp.zeros((micros, feat, rows), BF16), jnp.zeros((micros, n_chunk, CHUNK, rows), BF16), None)
    outs = []
    for t in range(main):
        incoming = shift(outs[t - SKEW], "section", 1, wrap=False) if t >= SKEW else None
        out, stash = forward(t, tab, patches, incoming, up, down, stash)
        outs.append(out)

    def forward_tail(t, carry):
        queue, stash = carry
        incoming = shift(queue[0], "section", 1, wrap=False)
        out, stash = forward(t, tab, patches, incoming, up, down, stash)
        return queue[1:] + (out,), stash

    _, stash = lax.fori_loop(main, ticks, forward_tail, (tuple(outs[-SKEW:]), stash))
    x_st, st_st, at_st, gp_st = stash

    back = (
        jnp.zeros((micros, rows, feat), BF16),
        jnp.zeros((micros, n_chunk, rows, CHUNK), BF16),
        jnp.zeros((micros, 8, feat), F32),
    )

    def backward_lead(t, carry):
        queue, back = carry
        out, back = backward(t, tab, cotangent, queue[0], up, down, x_st, gp_st, back)
        return queue[1:] + (shift(out, "section", -1, wrap=False),), back

    empty = tuple(jnp.zeros((rows, feat), BF16) for _ in range(SKEW))
    queue, back = lax.fori_loop(-lead, 0, backward_lead, (empty, back))
    queue = list(queue)
    for t in range(main):
        out, back = backward(t, tab, cotangent, queue[t], up, down, x_st, gp_st, back)
        if t + SKEW < main:
            queue.append(shift(out, "section", -1, wrap=False))
    g_st, gh_st, gg_st = back

    up_own, up_par, gain_own, gain_par = up_grads(place, st_st, gh_st, gg_st)
    down_own, down_par = down_grads(place, at_st, g_st)
    up_own = jnp.concatenate([up_own, gain_own], axis=3)
    up_par = jnp.concatenate([up_par, gain_par], axis=3)
    up_sum = scatter_sum(up_own, up_par, AX, AZ)
    down_sum = scatter_sum(down_own, down_par, AZ, AX)
    grad_up = up_sum[:, :hidden] * gain
    grad_gain = jnp.sum(up_sum[:, hidden:], axis=1) / gain[:, 0]
    return grad_up[None], down_sum[None], grad_gain[None]


def solution(mesh):
    finer = Mesh(
        mesh.devices.reshape(mesh.shape["section"], 4, 4, 2),
        ("section",) + FSDP,
    )
    in_specs = (
        P(None, FSDP, None),
        P(None, FSDP, None),
        P(),
        P(),
        P(),
        P("section", FSDP, None),
        P("section", FSDP, None),
        P("section", FSDP),
    )
    out_specs = (P("section", FSDP, None), P("section", FSDP, None), P("section", FSDP))
    return jax.shard_map(
        per_device, mesh=finer, in_specs=in_specs, out_specs=out_specs, check_vma=False
    )
```

```python
import functools

import jax
import jax.numpy as jnp
from jax import lax
from jax.experimental import pallas as pl
from jax.experimental.pallas import tpu as pltpu
from jax.sharding import Mesh
from jax.sharding import PartitionSpec as P

BLOCK = 128
EPSILON = 1e-05
AX, AZ, AC = "fsdp_0", "fsdp_1", "fsdp_2"
FSDP = (AX, AZ, AC)
SKEW = 2
GRANT = 36 << 20
CHUNK = 512
GELU_A = 0.7978845608028654
GELU_B = GELU_A * 0.044715
BF16, F32 = jnp.bfloat16, jnp.float32


ANY = pl.BlockSpec(memory_space=pl.ANY)
SMEM = pl.BlockSpec(memory_space=pltpu.SMEM)
VMEM = pl.BlockSpec(memory_space=pltpu.VMEM)


def shift(value, axis, distance, wrap=True):
    n = lax.axis_size(axis)
    if wrap:
        route = [(i, (i + distance) % n) for i in range(n)]
    else:
        route = [(i, i + distance) for i in range(n) if 0 <= i + distance < n]
    return lax.ppermute(value, axis, route)


def gather_pieces(own, first, second):
    line = jnp.stack([own] + [shift(own, first, -r) for r in (1, 2, 3)])
    ahead, behind = shift(line, second, -1), shift(line, second, 1)
    low = shift(behind[:2], second, 1)
    high = shift(ahead[2:], second, -1)
    mine = (line, ahead, behind, low, high)
    return mine + tuple(shift(p, AC, 1) for p in mine)


def placements(first_at, second_at, core):
    rows = []
    for own in (0, 1):
        c = core if own == 0 else 1 - core
        for piece, r2, r1s in ((0, 0, range(4)), (1, 1, range(4)), (2, 3, range(4)), (3, 2, (0, 1)), (4, 2, (2, 3))):
            for at, r1 in enumerate(r1s):
                rows.append((5 * own + piece, at, (first_at + r1) & 3, (second_at + r2) & 3, c))
    return rows


def assemble_kernel(place, *refs):
    ups, downs, (w_up, w_down, sem_up, sem_down) = refs[:10], refs[10:20], refs[20:]
    x, z, c = place[0], place[1], place[2]
    n_up, n_down = w_up.shape[0] // 32, w_down.shape[0] // 32
    copies = []
    for piece, at, fx, fz, core in placements(x, z, c):
        rows = pl.ds(pl.multiple_of((fx * 8 + fz * 2 + core) * n_up, n_up), n_up)
        copies.append(pltpu.make_async_copy(ups[piece].at[at], w_up.at[rows], sem_up.at[len(copies)]))
    late = []
    for piece, at, fz, fx, core in placements(z, x, c):
        rows = pl.ds(pl.multiple_of((fx * 8 + fz * 2 + core) * n_down, n_down), n_down)
        late.append(pltpu.make_async_copy(downs[piece].at[at], w_down.at[rows], sem_down.at[len(late)]))
    for copy in copies + late:
        copy.start()
    for copy in copies + late:
        copy.wait()


def gather_weights(up, down, place):
    ups = gather_pieces(up, AX, AZ)
    downs = gather_pieces(down, AZ, AX)
    return pl.pallas_call(
        assemble_kernel,
        out_shape=(
            pltpu.VMEM((32 * up.shape[0], up.shape[1]), BF16),
            pltpu.VMEM((32 * down.shape[0], down.shape[1]), BF16),
        ),
        in_specs=[SMEM] + [ANY] * 20,
        out_specs=(VMEM, VMEM),
        scratch_shapes=[pltpu.SemaphoreType.DMA((32,)), pltpu.SemaphoreType.DMA((32,))],
        compiler_params=pltpu.CompilerParams(vmem_limit_bytes=GRANT),
        name="assemble",
    )(place, *ups, *downs)


def norm_of(values, mask, width):
    mean = jnp.sum(values, axis=-1, keepdims=True) / width
    centered = jnp.where(mask, values - mean, 0.0)
    variance = jnp.sum(centered * centered, axis=-1, keepdims=True) / width
    inv_std = lax.rsqrt(variance + EPSILON)
    return centered * inv_std, inv_std


def held(value):
    return pltpu.with_memory_space_constraint(value, pltpu.VMEM)


def fetch(source, target, sem):
    copy = pltpu.make_async_copy(source, target, sem)
    copy.start()
    return copy


def forward_kernel(*refs, tick, has_input, aliased, micros):
    refs = list(refs)
    tab = refs.pop(0)
    if tick is None:
        tick = refs.pop(0)[0]
    patches = refs.pop(0)
    incoming = refs.pop(0) if has_input else None
    w_up, w_down = refs.pop(0), refs.pop(0)
    refs = refs[aliased:]
    out, x_st, st_st, at_st, gp_st = refs[:5]
    x_buf, st_buf, at_buf, gp_buf, acc, sem_x, sem_out, sem_st = refs[5:]
    n_chunk = at_buf.shape[0]
    sec = tab[4 * micros]
    q = tick - SKEW * sec
    at = jnp.clip(q, 0, micros - 1)
    micro, width, hidden, depth = tab[at], tab[micros + at], tab[2 * micros + at], tab[3 * micros + at]
    valid = jnp.logical_and(jnp.logical_and(q >= 0, q < micros), depth > sec)

    def chunk_of(c):
        return pl.ds(pl.multiple_of(c * CHUNK, CHUNK), CHUNK)

    def at_copy(c):
        return pltpu.make_async_copy(at_buf.at[c], at_st.at[at, c], sem_st.at[2 * c])

    def gp_copy(c):
        return pltpu.make_async_copy(gp_buf.at[c], gp_st.at[at, c], sem_st.at[2 * c + 1])

    @pl.when(valid)
    def run():
        used = (hidden + CHUNK - 1) // CHUNK
        if has_input:

            @pl.when(sec == 0)
            def first():
                fetch(patches.at[micro], x_buf, sem_x).wait()

            @pl.when(sec != 0)
            def later():
                fetch(incoming, x_buf, sem_x).wait()
        else:
            load = fetch(patches.at[micro], x_buf, sem_x)
        if not has_input:
            load.wait()
        mask = lax.broadcasted_iota(jnp.int32, x_buf.shape, 1) < width
        values = jnp.where(mask, x_buf[...].astype(F32), 0.0)
        x_buf[...] = values.astype(BF16)
        standard, _ = norm_of(values, mask, width.astype(F32))
        st_buf[...] = standard.T.astype(BF16)
        normed = standard.astype(BF16)
        copies = [fetch(x_buf, x_st.at[at], sem_out.at[0]), fetch(st_buf, st_st.at[at], sem_out.at[1])]
        acc[...] = values

        @pl.loop(0, used)
        def step(c):
            half = CHUNK // 2
            weight = w_up[:, chunk_of(c)]
            hids = [
                jnp.dot(normed, weight[:, j * half : (j + 1) * half], preferred_element_type=F32) for j in range(2)
            ]
            parts = []
            for j, h in enumerate(hids):
                h2 = h * h
                t = jnp.tanh(h * (GELU_A + GELU_B * h2))
                p = 0.5 + 0.5 * t
                act = h * p
                slope = p + act * (1.0 - t) * (GELU_A + (3.0 * GELU_B) * h2)
                unit = lax.broadcasted_iota(jnp.int32, h.shape, 1) + (c * CHUNK + j * half)
                inside = unit < hidden
                act = jnp.where(inside, act, 0.0)
                at_buf[c, j * half : (j + 1) * half, :] = act.T.astype(BF16)
                gp_buf[c, :, j * half : (j + 1) * half] = jnp.where(inside, slope, 0.0).astype(BF16)
                parts.append(act.astype(BF16))
            at_copy(c).start()
            gp_copy(c).start()
            acc[...] += jnp.dot(jnp.concatenate(parts, 1), w_down[chunk_of(c), :], preferred_element_type=F32)

        out[...] = jnp.where(mask, acc[...], 0.0).astype(BF16)

        @pl.loop(0, used)
        def drain(c):
            at_copy(c).wait()
            gp_copy(c).wait()

        for copy in copies:
            copy.wait()


def forward(tick, tab, patches, incoming, w_up, w_down, stash):
    micros, rows, feat = patches.shape
    n_chunk = w_up.shape[1] // CHUNK
    x_st, st_st, at_st, gp_st = stash
    slot = jax.ShapeDtypeStruct
    outs = (
        slot((rows, feat), BF16),
        slot((micros, rows, feat), BF16),
        slot((micros, feat, rows), BF16),
        slot((micros, n_chunk, CHUNK, rows), BF16),
        slot((micros, n_chunk, rows, CHUNK), BF16),
    )
    operands, specs = [tab], [SMEM]
    static = tick if isinstance(tick, int) else None
    if static is None:
        operands.append(tick.reshape(1))
        specs.append(SMEM)
    operands.append(patches)
    if incoming is not None:
        operands.append(incoming)
    specs += [ANY] * (len(operands) - len(specs)) + [VMEM] * 2
    operands += [held(w_up), held(w_down)]
    alias = {}
    aliased = 0
    for k, s in enumerate((x_st, st_st, at_st, gp_st)):
        if s is not None:
            alias[len(operands)] = k + 1
            operands.append(s)
            aliased += 1
    specs += [ANY] * (len(operands) - len(specs))
    body = functools.partial(
        forward_kernel, tick=static, has_input=incoming is not None, aliased=aliased, micros=micros
    )
    out, *stash = pl.pallas_call(
        body,
        out_shape=outs,
        in_specs=specs,
        out_specs=(VMEM, ANY, ANY, ANY, ANY),
        scratch_shapes=[
            pltpu.VMEM((rows, feat), BF16),
            pltpu.VMEM((feat, rows), BF16),
            pltpu.VMEM((n_chunk, CHUNK, rows), BF16),
            pltpu.VMEM((n_chunk, rows, CHUNK), BF16),
            pltpu.VMEM((rows, feat), F32),
            pltpu.SemaphoreType.DMA,
            pltpu.SemaphoreType.DMA((2,)),
            pltpu.SemaphoreType.DMA((2 * n_chunk,)),
        ],
        input_output_aliases=alias,
        compiler_params=pltpu.CompilerParams(vmem_limit_bytes=GRANT),
        name="forward",
    )(*operands)
    return out, tuple(stash)


def backward_kernel(*refs, tick, micros):
    refs = list(refs)
    tab = refs.pop(0)
    if tick is None:
        tick = refs.pop(0)[0]
    cotangent, incoming, w_up, w_down, x_st, gp_st = refs[:6]
    refs = refs[9:]
    out, g_st, gh_st, gg_st = refs[:4]
    x_buf, g_buf, gp_buf, gh_buf, gg_buf, acc, sem_g, sem_x, sem_out, sem_gp, sem_gh = refs[4:]
    n_chunk = gp_buf.shape[0]
    sec = tab[4 * micros]
    q = (micros - 1) - (tick + SKEW * (sec - 1))
    at = jnp.clip(q, 0, micros - 1)
    micro, width, hidden, depth = tab[at], tab[micros + at], tab[2 * micros + at], tab[3 * micros + at]
    valid = jnp.logical_and(jnp.logical_and(q >= 0, q < micros), depth > sec)

    def chunk_of(c):
        return pl.ds(pl.multiple_of(c * CHUNK, CHUNK), CHUNK)

    def gp_copy(c):
        return pltpu.make_async_copy(gp_st.at[at, c], gp_buf.at[c], sem_gp.at[c])

    def gh_copy(c):
        return pltpu.make_async_copy(gh_buf.at[c], gh_st.at[at, c], sem_gh.at[c])

    @pl.when(valid)
    def run():
        used = (hidden + CHUNK - 1) // CHUNK
        load_x = fetch(x_st.at[at], x_buf, sem_x)

        @pl.loop(0, used)
        def load(c):
            gp_copy(c).start()

        @pl.when(depth == sec + 1)
        def last():
            fetch(cotangent.at[micro], g_buf, sem_g).wait()

        @pl.when(depth != sec + 1)
        def inner():
            fetch(incoming, g_buf, sem_g).wait()

        mask = lax.broadcasted_iota(jnp.int32, x_buf.shape, 1) < width
        grad_out = jnp.where(mask, g_buf[...].astype(F32), 0.0)
        g_buf[...] = grad_out.astype(BF16)
        grad_branch = g_buf[...]
        copies = [fetch(g_buf, g_st.at[at], sem_out.at[0])]
        acc[...] = jnp.zeros(acc.shape, F32)

        @pl.loop(0, used)
        def step(c):
            nt = (((1,), (1,)), ((), ()))
            grad_act = lax.dot_general(grad_branch, w_down[chunk_of(c), :], nt, preferred_element_type=F32)
            gp_copy(c).wait()
            grad_hid = (grad_act * gp_buf[c].astype(F32)).astype(BF16)
            gh_buf[c] = grad_hid
            gh_copy(c).start()
            acc[...] += lax.dot_general(grad_hid, w_up[:, chunk_of(c)], nt, preferred_element_type=F32)

        load_x.wait()
        width_float = width.astype(F32)
        standard, inv_std = norm_of(x_buf[...].astype(F32), mask, width_float)
        grad_std = jnp.where(mask, acc[...], 0.0)
        product = grad_std * standard
        gg_buf[...] = jnp.sum(product.reshape(-1, 8, product.shape[1]), axis=0)
        copies.append(fetch(gg_buf, gg_st.at[at], sem_out.at[1]))
        first_mean = jnp.sum(grad_std, axis=-1, keepdims=True) / width_float
        second_mean = jnp.sum(product, axis=-1, keepdims=True) / width_float
        grad_in = inv_std * (grad_std - first_mean - standard * second_mean)
        out[...] = jnp.where(mask, grad_out + grad_in, 0.0).astype(BF16)

        @pl.loop(0, used)
        def drain(c):
            gh_copy(c).wait()

        for copy in copies:
            copy.wait()


def backward(tick, tab, cotangent, incoming, w_up, w_down, x_st, gp_st, stash):
    micros, rows, feat = cotangent.shape
    n_chunk = w_up.shape[1] // CHUNK
    slot = jax.ShapeDtypeStruct
    operands, specs = [tab], [SMEM]
    static = tick if isinstance(tick, int) else None
    if static is None:
        operands.append(tick.reshape(1))
        specs.append(SMEM)
    operands += [cotangent, incoming, held(w_up), held(w_down), x_st, gp_st]
    specs += [ANY, ANY, VMEM, VMEM]
    alias = {len(operands) + k: k + 1 for k in range(3)}
    operands += list(stash)
    specs += [ANY] * (len(operands) - len(specs))
    out, *stash = pl.pallas_call(
        functools.partial(backward_kernel, tick=static, micros=micros),
        out_shape=(
            slot((rows, feat), BF16),
            slot((micros, rows, feat), BF16),
            slot((micros, n_chunk, rows, CHUNK), BF16),
            slot((micros, 8, feat), F32),
        ),
        in_specs=specs,
        out_specs=(VMEM, ANY, ANY, ANY),
        scratch_shapes=[
            pltpu.VMEM((rows, feat), BF16),
            pltpu.VMEM((rows, feat), BF16),
            pltpu.VMEM((n_chunk, rows, CHUNK), BF16),
            pltpu.VMEM((n_chunk, rows, CHUNK), BF16),
            pltpu.VMEM((8, feat), F32),
            pltpu.VMEM((rows, feat), F32),
            pltpu.SemaphoreType.DMA,
            pltpu.SemaphoreType.DMA,
            pltpu.SemaphoreType.DMA((2,)),
            pltpu.SemaphoreType.DMA((n_chunk,)),
            pltpu.SemaphoreType.DMA((n_chunk,)),
        ],
        input_output_aliases=alias,
        compiler_params=pltpu.CompilerParams(vmem_limit_bytes=GRANT),
        name="backward",
    )(*operands)
    return out, tuple(stash)


def split_cores(core, blocks, mine, theirs, value_of):
    for parity, targets in ((0, (mine, theirs)), (1, (theirs, mine))):

        @pl.when(core == parity)
        def write(targets=targets):
            for f in range(blocks):
                targets[f & 1](f >> 3, (f >> 1) & 3, value_of(f))


def up_kernel(place, st, gh, gg, up_own, up_par, gain_own, gain_par):
    x, z, core = place[0], place[1], place[2]
    micros = st.shape[0]

    def put(ref):
        def write(fx, fz, value):
            ref[(fx - x) & 3, (fz - z) & 3] = value

        return write

    left = jnp.concatenate([st[i] for i in range(micros)], axis=1)
    right = jnp.concatenate([gh[i, 0] for i in range(micros)], axis=0)
    up = jnp.dot(left, right, preferred_element_type=F32).astype(BF16)
    n = up.shape[0] // 32
    split_cores(core, 32, put(up_own), put(up_par), lambda f: up[f * n : (f + 1) * n])

    @pl.when(pl.program_id(0) == 0)
    def gains():
        total = gg[...].reshape(-1, gg.shape[2])
        total = jnp.concatenate([total, jnp.zeros((128 - total.shape[0], total.shape[1]), F32)], axis=0)
        column = total.T.astype(BF16)
        split_cores(core, 32, put(gain_own), put(gain_par), lambda f: column[f * n : (f + 1) * n])


def up_grads(place, st_st, gh_st, gg_st):
    micros, feat, rows = st_st.shape
    n_chunk = gh_st.shape[1]
    part = feat // 32
    wide = jax.ShapeDtypeStruct((4, 4, part, n_chunk * CHUNK), BF16)
    thin = jax.ShapeDtypeStruct((4, 4, part, 128), BF16)
    wide_spec = pl.BlockSpec((4, 4, part, CHUNK), lambda c: (0, 0, 0, c))
    thin_spec = pl.BlockSpec((4, 4, part, 128), lambda c: (0, 0, 0, 0))
    return pl.pallas_call(
        up_kernel,
        grid=(n_chunk,),
        out_shape=(wide, wide, thin, thin),
        in_specs=[
            SMEM,
            pl.BlockSpec((micros, feat, rows), lambda c: (0, 0, 0)),
            pl.BlockSpec((micros, 1, rows, CHUNK), lambda c: (0, c, 0, 0)),
            pl.BlockSpec(gg_st.shape, lambda c: (0, 0, 0)),
        ],
        out_specs=(wide_spec, wide_spec, thin_spec, thin_spec),
        name="up_grads",
    )(place, st_st, gh_st, gg_st)


def down_kernel(place, at, g, own, par):
    core, z = place[2], place[1]
    micros = at.shape[0]
    right = g[...].reshape(-1, g.shape[2])
    left = jnp.concatenate([at[i].reshape(-1, at.shape[3]) for i in range(micros)], axis=1)
    down = jnp.dot(left, right, preferred_element_type=F32).astype(BF16)
    n = down.shape[0] // 8
    for parity, targets in ((0, (own, par)), (1, (par, own))):

        @pl.when(core == parity)
        def write(targets=targets):
            for f in range(8):
                targets[f & 1][((f >> 1) - z) & 3, 0] = down[f * n : (f + 1) * n]


def down_grads(place, at_st, g_st):
    micros, n_chunk, _, rows = at_st.shape
    feat = g_st.shape[2]
    wide = n_chunk * CHUNK // 4
    unit = 256
    at_view = at_st.reshape(micros, n_chunk * CHUNK // unit, unit, rows)
    part = n_chunk * CHUNK // 32
    out = jax.ShapeDtypeStruct((4, 4, part, feat), BF16)
    spec = pl.BlockSpec((4, 1, part, feat), lambda i, p: (0, (i - p[0]) & 3, 0, 0))
    return pl.pallas_call(
        down_kernel,
        grid_spec=pltpu.PrefetchScalarGridSpec(
            num_scalar_prefetch=1,
            grid=(4,),
            in_specs=[
                pl.BlockSpec((micros, wide // unit, unit, rows), lambda i, p: (0, i, 0, 0)),
                pl.BlockSpec(g_st.shape, lambda i, p: (0, 0, 0)),
            ],
            out_specs=(spec, spec),
        ),
        out_shape=(out, out),
        name="down_grads",
    )(place, at_view, g_st)


def plus(*values):
    total = values[0].astype(F32)
    for v in values[1:]:
        total = total + v.astype(F32)
    return total


def scatter_sum(own, partner, first, second):
    other = shift(partner, AC, 1)

    def joined(*at):
        return plus(own[at], other[at])

    low = shift(joined(2, slice(0, 2)).astype(BF16), first, 1)
    high = shift(joined(2, slice(2, 4)).astype(BF16), first, -1)
    ahead = jnp.concatenate([plus(joined(1, slice(0, 2)), low), joined(1, slice(2, 4))]).astype(BF16)
    behind = jnp.concatenate([joined(3, slice(0, 2)), plus(joined(3, slice(2, 4)), high)]).astype(BF16)
    line = plus(joined(0), shift(ahead, first, 1), shift(behind, first, -1))
    parts = [shift(line[r].astype(BF16), second, r) for r in (1, 2, 3)]
    return plus(line[0], *parts)


def schedule_table(embed_blocks, ratio_index, depth):
    micros = depth.shape[0]
    index = lax.iota(jnp.int32, micros)
    before = jnp.logical_or(
        depth[None, :] > depth[:, None],
        jnp.logical_and(depth[None, :] == depth[:, None], index[None, :] < index[:, None]),
    )
    rank = jnp.sum(before.astype(jnp.int32), axis=1)
    chosen = rank[None, :] == index[:, None]
    width = embed_blocks * BLOCK
    hidden = width * (6 + ratio_index) // 2
    columns = jnp.stack([index, width, hidden, depth])
    table = jnp.sum(jnp.where(chosen[None], columns[:, None, :], 0), axis=2)
    section = lax.axis_index("section").astype(jnp.int32)
    return jnp.concatenate([table.reshape(-1), jnp.full((8,), section, jnp.int32)])


def per_device(patches, cotangent, embed_blocks, ratio_index, depth, w_up, w_down, ln_gain):
    sections = lax.axis_size("section")
    micros, rows, feat = patches.shape
    hidden = w_up.shape[2]
    n_chunk = hidden // CHUNK
    gain = ln_gain[0].astype(F32)[:, None]
    place = jnp.stack([lax.axis_index(a) for a in FSDP]).astype(jnp.int32)
    tab = schedule_table(embed_blocks, ratio_index, depth)
    scaled = (w_up[0].astype(F32) * gain).astype(BF16)
    up, down = gather_weights(scaled, w_down[0], place)

    reach = [jnp.sum((depth > s).astype(jnp.int32)) for s in range(sections)]
    main = micros + SKEW
    ticks = functools.reduce(jnp.maximum, [n + SKEW * s for s, n in enumerate(reach) if s > 1], main)
    lead = functools.reduce(
        jnp.maximum, [n + SKEW * (s - 1) for s, n in enumerate(reach) if s > 1], micros
    ) - micros

    stash = (None, jnp.zeros((micros, feat, rows), BF16), jnp.zeros((micros, n_chunk, CHUNK, rows), BF16), None)
    outs = []
    for t in range(main):
        incoming = shift(outs[t - SKEW], "section", 1, wrap=False) if t >= SKEW else None
        out, stash = forward(t, tab, patches, incoming, up, down, stash)
        outs.append(out)

    def forward_tail(t, carry):
        queue, stash = carry
        incoming = shift(queue[0], "section", 1, wrap=False)
        out, stash = forward(t, tab, patches, incoming, up, down, stash)
        return queue[1:] + (out,), stash

    _, stash = lax.fori_loop(main, ticks, forward_tail, (tuple(outs[-SKEW:]), stash))
    x_st, st_st, at_st, gp_st = stash

    back = (
        jnp.zeros((micros, rows, feat), BF16),
        jnp.zeros((micros, n_chunk, rows, CHUNK), BF16),
        jnp.zeros((micros, 8, feat), F32),
    )

    def backward_lead(t, carry):
        queue, back = carry
        out, back = backward(t, tab, cotangent, queue[0], up, down, x_st, gp_st, back)
        return queue[1:] + (shift(out, "section", -1, wrap=False),), back

    empty = tuple(jnp.zeros((rows, feat), BF16) for _ in range(SKEW))
    queue, back = lax.fori_loop(-lead, 0, backward_lead, (empty, back))
    queue = list(queue)
    for t in range(main):
        out, back = backward(t, tab, cotangent, queue[t], up, down, x_st, gp_st, back)
        if t + SKEW < main:
            queue.append(shift(out, "section", -1, wrap=False))
    g_st, gh_st, gg_st = back

    up_own, up_par, gain_own, gain_par = up_grads(place, st_st, gh_st, gg_st)
    down_own, down_par = down_grads(place, at_st, g_st)
    up_own = jnp.concatenate([up_own, gain_own], axis=3)
    up_par = jnp.concatenate([up_par, gain_par], axis=3)
    up_sum = scatter_sum(up_own, up_par, AX, AZ)
    down_sum = scatter_sum(down_own, down_par, AZ, AX)
    grad_up = up_sum[:, :hidden] * gain
    grad_gain = jnp.sum(up_sum[:, hidden:], axis=1) / gain[:, 0]
    return grad_up[None], down_sum[None], grad_gain[None]


def solution(mesh):
    finer = Mesh(
        mesh.devices.reshape(mesh.shape["section"], 4, 4, 2),
        ("section",) + FSDP,
    )
    in_specs = (
        P(None, FSDP, None),
        P(None, FSDP, None),
        P(),
        P(),
        P(),
        P("section", FSDP, None),
        P("section", FSDP, None),
        P("section", FSDP),
    )
    out_specs = (P("section", FSDP, None), P("section", FSDP, None), P("section", FSDP))
    return jax.shard_map(
        per_device, mesh=finer, in_specs=in_specs, out_specs=out_specs, check_vma=False
    )
```

```python
import functools

import jax
import jax.numpy as jnp
from jax import lax
from jax.experimental import pallas as pl
from jax.experimental.pallas import tpu as pltpu
from jax.sharding import Mesh
from jax.sharding import PartitionSpec as P

BLOCK = 128
EPSILON = 1e-05
AX, AZ, AC = "fsdp_0", "fsdp_1", "fsdp_2"
FSDP = (AX, AZ, AC)
SKEW = 2
GRANT = 16 << 20
CHUNK = 256
GRAD_CHUNK = 512
GELU_A = 0.7978845608028654
GELU_B = GELU_A * 0.044715
BF16, F32 = jnp.bfloat16, jnp.float32


HBM = pl.BlockSpec(memory_space=pltpu.HBM)
SMEM = pl.BlockSpec(memory_space=pltpu.SMEM)
VMEM = pl.BlockSpec(memory_space=pltpu.VMEM)


def shift(value, axis, distance, wrap=True):
    n = lax.axis_size(axis)
    if wrap:
        route = [(i, (i + distance) % n) for i in range(n)]
    else:
        route = [(i, i + distance) for i in range(n) if 0 <= i + distance < n]
    return lax.ppermute(value, axis, route)


def gather_pieces(own, first, second):
    line = jnp.stack([own] + [shift(own, first, -r) for r in (1, 2, 3)])
    ahead, behind = shift(line, second, -1), shift(line, second, 1)
    low = shift(behind[:2], second, 1)
    high = shift(ahead[2:], second, -1)
    mine = (line, ahead, behind, low, high)
    return mine + tuple(shift(p, AC, 1) for p in mine)


def placements(first_at, second_at, core):
    rows = []
    for own in (0, 1):
        c = core if own == 0 else 1 - core
        for piece, r2, r1s in ((0, 0, range(4)), (1, 1, range(4)), (2, 3, range(4)), (3, 2, (0, 1)), (4, 2, (2, 3))):
            for at, r1 in enumerate(r1s):
                rows.append((5 * own + piece, at, (first_at + r1) & 3, (second_at + r2) & 3, c))
    return rows


def assemble_kernel(place, *refs):
    ups, downs = refs[:10], refs[10:20]
    w_up, w_down, x_st, st_st, at_st, gp_st, g_st, gh_st, gg_st, sem_up, sem_down = refs[20:]
    x, z, c = place[0], place[1], place[2]
    n_up, n_down = w_up.shape[0] // 32, w_down.shape[0] // 32
    copies = []
    for piece, at, fx, fz, core in placements(x, z, c):
        rows = pl.ds(pl.multiple_of((fx * 8 + fz * 2 + core) * n_up, n_up), n_up)
        copies.append(pltpu.make_async_copy(ups[piece].at[at], w_up.at[rows], sem_up.at[len(copies)]))
    late = []
    for piece, at, fz, fx, core in placements(z, x, c):
        rows = pl.ds(pl.multiple_of((fx * 8 + fz * 2 + core) * n_down, n_down), n_down)
        late.append(pltpu.make_async_copy(downs[piece].at[at], w_down.at[rows], sem_down.at[len(late)]))
    for copy in copies + late:
        copy.start()
    for ref in (st_st, at_st, g_st, gh_st, gg_st):

        @pl.loop(0, ref.shape[0] // 64)
        def clear(i, ref=ref):
            ref[pl.ds(pl.multiple_of(i * 64, 64), 64), :] = jnp.zeros((64, ref.shape[1]), ref.dtype)

    for copy in copies + late:
        copy.wait()


def assemble(place, ups, downs, micros, rows):
    feat, hidden, tokens = 32 * ups[0].shape[1], ups[0].shape[2], micros * rows
    shapes = (
        (feat, hidden),
        (hidden, feat),
        (tokens, feat),
        (feat, tokens),
        (hidden, tokens),
        (tokens, hidden),
        (tokens, feat),
        (tokens, hidden),
    )
    return pl.pallas_call(
        assemble_kernel,
        out_shape=tuple(pltpu.VMEM(s, BF16) for s in shapes) + (pltpu.VMEM((8 * micros, feat), F32),),
        in_specs=[SMEM] + [HBM] * 20,
        out_specs=(VMEM,) * 9,
        scratch_shapes=[pltpu.SemaphoreType.DMA((32,)), pltpu.SemaphoreType.DMA((32,))],
        compiler_params=pltpu.CompilerParams(vmem_limit_bytes=GRANT),
        name="assemble",
    )(place, *[pltpu.with_memory_space_constraint(v, pltpu.HBM) for v in ups + downs])


def norm_of(values, mask, width):
    mean = jnp.sum(values, axis=-1, keepdims=True) / width
    centered = jnp.where(mask, values - mean, 0.0)
    variance = jnp.sum(centered * centered, axis=-1, keepdims=True) / width
    inv_std = lax.rsqrt(variance + EPSILON)
    return centered * inv_std, inv_std


def held(value):
    return pltpu.with_memory_space_constraint(value, pltpu.VMEM)


def span(index, size):
    return pl.ds(pl.multiple_of(index * size, size), size)


def job_of(tab, q, micros):
    sec = tab[4 * micros]
    at = jnp.clip(q, 0, micros - 1)
    micro, width, hidden, depth = tab[at], tab[micros + at], tab[2 * micros + at], tab[3 * micros + at]
    valid = jnp.logical_and(jnp.logical_and(q >= 0, q < micros), depth > sec)
    return sec, at, micro, width, hidden, depth, valid


def forward_kernel(tab, patches, incoming, w_up, w_down, _x, _st, _at, _gp, *refs, tick):
    out, x_st, st_st, at_st, gp_st, normed, hid_buf, act_buf, acc = refs
    micros, rows, _ = patches.shape
    sec, at, micro, width, hidden, _, valid = job_of(tab, tick - SKEW * tab[4 * micros], micros)

    @pl.when(valid)
    def run():
        used = (hidden + CHUNK - 1) // CHUNK
        mine = span(at, rows)

        @pl.when(sec == 0)
        def first():
            acc[...] = patches[micro].astype(F32)

        @pl.when(sec != 0)
        def later():
            acc[...] = incoming[...].astype(F32)

        mask = lax.broadcasted_iota(jnp.int32, acc.shape, 1) < width
        values = jnp.where(mask, acc[...], 0.0)
        acc[...] = values
        x_st[mine, :] = values.astype(BF16)
        standard, _ = norm_of(values, mask, width.astype(F32))
        normed[...] = standard.astype(BF16)
        st_st[:, mine] = standard.T.astype(BF16)
        act_buf[...] = jnp.zeros(act_buf.shape, BF16)
        hid_buf[...] = jnp.dot(normed[...], w_up[:, :CHUNK], preferred_element_type=F32)

        @pl.loop(0, used)
        def step(c):
            h, ready = hid_buf[...], act_buf[...]
            following = jnp.minimum(c + 1, used - 1)
            hid_next = jnp.dot(normed[...], w_up[:, span(following, CHUNK)], preferred_element_type=F32)
            before = jnp.maximum(c - 1, 0)
            acc[...] += jnp.dot(ready, w_down[span(before, CHUNK), :], preferred_element_type=F32)
            h2 = h * h
            t = jnp.tanh(h * (GELU_A + GELU_B * h2))
            p = 0.5 + 0.5 * t
            act = h * p
            slope = p + act * (1.0 - t) * (GELU_A + (3.0 * GELU_B) * h2)
            inside = lax.broadcasted_iota(jnp.int32, h.shape, 1) < hidden - c * CHUNK
            act = jnp.where(inside, act, 0.0)
            act_buf[...] = act.astype(BF16)
            at_st[span(c, CHUNK), mine] = act.T.astype(BF16)
            gp_st[mine, span(c, CHUNK)] = jnp.where(inside, slope, 0.0).astype(BF16)
            hid_buf[...] = hid_next

        total = acc[...] + jnp.dot(act_buf[...], w_down[span(used - 1, CHUNK), :], preferred_element_type=F32)
        out[...] = jnp.where(mask, total, 0.0).astype(BF16)


def forward(tick, tab, patches, incoming, w_up, w_down, stash):
    _, rows, feat = patches.shape
    operands = [tab, held(patches), held(incoming), held(w_up), held(w_down)] + [held(s) for s in stash]
    out, *stash = pl.pallas_call(
        functools.partial(forward_kernel, tick=tick),
        out_shape=(jax.ShapeDtypeStruct((rows, feat), BF16),) + tuple(pltpu.VMEM(s.shape, s.dtype) for s in stash),
        in_specs=[SMEM] + [VMEM] * 8,
        out_specs=(VMEM,) * 5,
        scratch_shapes=[
            pltpu.VMEM((rows, feat), BF16),
            pltpu.VMEM((rows, CHUNK), F32),
            pltpu.VMEM((rows, CHUNK), BF16),
            pltpu.VMEM((rows, feat), F32),
        ],
        input_output_aliases={5 + k: 1 + k for k in range(4)},
        compiler_params=pltpu.CompilerParams(vmem_limit_bytes=GRANT),
        name="forward",
    )(*operands)
    return out, tuple(stash)


def backward_kernel(tab, cotangent, incoming, w_up, w_down, x_st, gp_st, _g, _gh, _gg, *refs, tick):
    out, g_st, gh_st, gg_st, g_buf, gh_buf, acc = refs
    micros, rows, _ = cotangent.shape
    q = (micros - 1) - (tick + SKEW * (tab[4 * micros] - 1))
    sec, at, micro, width, hidden, depth, valid = job_of(tab, q, micros)

    @pl.when(valid)
    def run():
        used = (hidden + CHUNK - 1) // CHUNK
        mine = span(at, rows)

        @pl.when(depth == sec + 1)
        def last():
            g_buf[...] = cotangent[micro]

        @pl.when(depth != sec + 1)
        def inner():
            g_buf[...] = incoming[...]

        mask = lax.broadcasted_iota(jnp.int32, acc.shape, 1) < width
        grad_branch = jnp.where(mask, g_buf[...].astype(F32), 0.0).astype(BF16)
        g_buf[...] = grad_branch
        g_st[mine, :] = grad_branch
        acc[...] = jnp.zeros(acc.shape, F32)
        gh_buf[...] = jnp.zeros(gh_buf.shape, BF16)
        nt = (((1,), (1,)), ((), ()))

        @pl.loop(0, used)
        def step(c):
            ready = gh_buf[...]
            grad_act = lax.dot_general(g_buf[...], w_down[span(c, CHUNK), :], nt, preferred_element_type=F32)
            before = jnp.maximum(c - 1, 0)
            acc[...] += lax.dot_general(ready, w_up[:, span(before, CHUNK)], nt, preferred_element_type=F32)
            grad_hid = (grad_act * gp_st[mine, span(c, CHUNK)].astype(F32)).astype(BF16)
            gh_buf[...] = grad_hid
            gh_st[mine, span(c, CHUNK)] = grad_hid

        total = acc[...] + lax.dot_general(
            gh_buf[...], w_up[:, span(used - 1, CHUNK)], nt, preferred_element_type=F32
        )
        width_float = width.astype(F32)
        standard, inv_std = norm_of(x_st[mine, :].astype(F32), mask, width_float)
        grad_std = jnp.where(mask, total, 0.0)
        product = grad_std * standard
        gg_st[span(at, 8), :] = jnp.sum(product.reshape(-1, 8, product.shape[1]), axis=0)
        first_mean = jnp.sum(grad_std, axis=-1, keepdims=True) / width_float
        second_mean = jnp.sum(product, axis=-1, keepdims=True) / width_float
        grad_in = inv_std * (grad_std - first_mean - standard * second_mean)
        out[...] = jnp.where(mask, g_buf[...].astype(F32) + grad_in, 0.0).astype(BF16)


def backward(tick, tab, cotangent, incoming, w_up, w_down, x_st, gp_st, stash):
    _, rows, feat = cotangent.shape
    operands = [tab] + [held(v) for v in (cotangent, incoming, w_up, w_down, x_st, gp_st) + tuple(stash)]
    out, *stash = pl.pallas_call(
        functools.partial(backward_kernel, tick=tick),
        out_shape=(jax.ShapeDtypeStruct((rows, feat), BF16),) + tuple(pltpu.VMEM(s.shape, s.dtype) for s in stash),
        in_specs=[SMEM] + [VMEM] * 9,
        out_specs=(VMEM,) * 4,
        scratch_shapes=[
            pltpu.VMEM((rows, feat), BF16),
            pltpu.VMEM((rows, CHUNK), BF16),
            pltpu.VMEM((rows, feat), F32),
        ],
        input_output_aliases={7 + k: 1 + k for k in range(3)},
        compiler_params=pltpu.CompilerParams(vmem_limit_bytes=GRANT),
        name="backward",
    )(*operands)
    return out, tuple(stash)


def split_cores(core, blocks, mine, theirs, value_of):
    for parity, targets in ((0, (mine, theirs)), (1, (theirs, mine))):

        @pl.when(core == parity)
        def write(targets=targets):
            for f in range(blocks):
                targets[f & 1](f >> 3, (f >> 1) & 3, value_of(f))


def up_kernel(place, st, gh, gg, own, par):
    x, z, core = place[0], place[1], place[2]
    hidden = gh.shape[1]
    n = st.shape[0] // 32

    def put(ref, columns):
        def write(fx, fz, value):
            ref[(fx - x) & 3, (fz - z) & 3, :, columns] = value

        return write

    @pl.loop(0, hidden // GRAD_CHUNK)
    def step(c):
        columns = span(c, GRAD_CHUNK)
        up = jnp.dot(st[...], gh[:, columns], preferred_element_type=F32).astype(BF16)
        split_cores(core, 32, put(own, columns), put(par, columns), lambda f: up[f * n : (f + 1) * n])

    total = gg[...]
    total = jnp.concatenate([total, jnp.zeros((128 - total.shape[0], total.shape[1]), F32)], axis=0)
    column = total.T.astype(BF16)
    last = pl.ds(hidden, 128)
    split_cores(core, 32, put(own, last), put(par, last), lambda f: column[f * n : (f + 1) * n])


def up_grads(place, st_st, gh_st, gg_st):
    feat, hidden = st_st.shape[0], gh_st.shape[1]
    out = jax.ShapeDtypeStruct((4, 4, feat // 32, hidden + 128), BF16)
    return pl.pallas_call(
        up_kernel,
        out_shape=(out, out),
        in_specs=[SMEM] + [VMEM] * 3,
        out_specs=(VMEM, VMEM),
        compiler_params=pltpu.CompilerParams(vmem_limit_bytes=GRANT),
        name="up_grads",
    )(place, held(st_st), held(gh_st), held(gg_st))


def down_kernel(place, at, g, own, par):
    x, z, core = place[0], place[1], place[2]
    n = at.shape[0] // 32

    @pl.loop(0, 4)
    def step(i):
        down = jnp.dot(at[span(i, 8 * n), :], g[...], preferred_element_type=F32).astype(BF16)
        for parity, targets in ((0, (own, par)), (1, (par, own))):

            @pl.when(core == parity)
            def write(targets=targets):
                for f in range(8):
                    targets[f & 1][((f >> 1) - z) & 3, (i - x) & 3] = down[f * n : (f + 1) * n]


def down_grads(place, at_st, g_st):
    out = jax.ShapeDtypeStruct((4, 4, at_st.shape[0] // 32, g_st.shape[1]), BF16)
    return pl.pallas_call(
        down_kernel,
        out_shape=(out, out),
        in_specs=[SMEM] + [VMEM] * 2,
        out_specs=(VMEM, VMEM),
        compiler_params=pltpu.CompilerParams(vmem_limit_bytes=GRANT),
        name="down_grads",
    )(place, held(at_st), held(g_st))


def plus(*values):
    total = values[0].astype(F32)
    for v in values[1:]:
        total = total + v.astype(F32)
    return total


def scatter_sum(own, partner, first, second):
    other = shift(partner, AC, 1)

    def joined(*at):
        return plus(own[at], other[at])

    low = shift(joined(2, slice(0, 2)).astype(BF16), first, 1)
    high = shift(joined(2, slice(2, 4)).astype(BF16), first, -1)
    ahead = jnp.concatenate([plus(joined(1, slice(0, 2)), low), joined(1, slice(2, 4))]).astype(BF16)
    behind = jnp.concatenate([joined(3, slice(0, 2)), plus(joined(3, slice(2, 4)), high)]).astype(BF16)
    line = plus(joined(0), shift(ahead, first, 1), shift(behind, first, -1))
    parts = [shift(line[r].astype(BF16), second, r) for r in (1, 2, 3)]
    return plus(line[0], *parts)


def schedule_table(embed_blocks, ratio_index, depth):
    micros = depth.shape[0]
    index = lax.iota(jnp.int32, micros)
    before = jnp.logical_or(
        depth[None, :] > depth[:, None],
        jnp.logical_and(depth[None, :] == depth[:, None], index[None, :] < index[:, None]),
    )
    rank = jnp.sum(before.astype(jnp.int32), axis=1)
    chosen = rank[None, :] == index[:, None]
    width = embed_blocks * BLOCK
    hidden = width * (6 + ratio_index) // 2
    columns = jnp.stack([index, width, hidden, depth])
    table = jnp.sum(jnp.where(chosen[None], columns[:, None, :], 0), axis=2)
    section = lax.axis_index("section").astype(jnp.int32)
    return jnp.concatenate([table.reshape(-1), jnp.full((8,), section, jnp.int32)])


def window(extra, tab, place, gain, patches, cotangent, ups, downs):
    micros, rows, _ = patches.shape
    up, down, *stash, g_st, gh_st, gg_st = assemble(place, ups, downs, micros, rows)
    hidden = up.shape[1]
    main = micros + SKEW

    outs = []
    for t in range(main + extra):
        incoming = shift(outs[t - SKEW], "section", 1, wrap=False) if t >= SKEW else patches[0]
        out, stash = forward(t, tab, patches, incoming, up, down, stash)
        outs.append(out)
    x_st, st_st, at_st, gp_st = stash

    back = (g_st, gh_st, gg_st)
    outs = []
    for t in range(main + extra):
        incoming = shift(outs[t - SKEW], "section", -1, wrap=False) if t >= SKEW else cotangent[0]
        out, back = backward(t - extra, tab, cotangent, incoming, up, down, x_st, gp_st, back)
        outs.append(out)
    g_st, gh_st, gg_st = back

    down_own, down_par = down_grads(place, at_st, g_st)
    up_own, up_par = up_grads(place, st_st, gh_st, gg_st)
    down_sum = scatter_sum(down_own, down_par, AZ, AX)
    up_sum = scatter_sum(up_own, up_par, AX, AZ)
    grad_up = up_sum[:, :hidden] * gain
    grad_gain = jnp.sum(up_sum[:, hidden:], axis=1) / gain[:, 0]
    return grad_up, down_sum, grad_gain


def per_device(patches, cotangent, embed_blocks, ratio_index, depth, w_up, w_down, ln_gain):
    sections = lax.axis_size("section")
    micros = patches.shape[0]
    gain = ln_gain[0].astype(F32)[:, None]
    place = jnp.stack([lax.axis_index(a) for a in FSDP]).astype(jnp.int32)
    tab = schedule_table(embed_blocks, ratio_index, depth)
    scaled = (w_up[0].astype(F32) * gain).astype(BF16)
    ups = gather_pieces(scaled, AX, AZ)
    downs = gather_pieces(w_down[0], AZ, AX)

    is_deep = jnp.zeros((), bool)
    for s in range(2, sections):
        reach = jnp.sum((depth > s).astype(jnp.int32))
        is_deep = jnp.logical_or(is_deep, reach > micros - SKEW * (s - 1))
    results = lax.cond(
        is_deep,
        functools.partial(window, SKEW * (sections - 2)),
        functools.partial(window, 0),
        *(tab, place, gain, patches, cotangent, ups, downs),
    )
    return tuple(r[None] for r in results)


def solution(mesh):
    finer = Mesh(
        mesh.devices.reshape(mesh.shape["section"], 4, 4, 2),
        ("section",) + FSDP,
    )
    in_specs = (
        P(None, FSDP, None),
        P(None, FSDP, None),
        P(),
        P(),
        P(),
        P("section", FSDP, None),
        P("section", FSDP, None),
        P("section", FSDP),
    )
    out_specs = (P("section", FSDP, None), P("section", FSDP, None), P("section", FSDP))
    return jax.shard_map(
        per_device, mesh=finer, in_specs=in_specs, out_specs=out_specs, check_vma=False
    )
```

```python
import functools

import jax
import jax.numpy as jnp
from jax import lax
from jax.experimental import pallas as pl
from jax.experimental.pallas import tpu as pltpu
from jax.sharding import Mesh
from jax.sharding import PartitionSpec as P

BLOCK = 128
EPSILON = 1e-05
AX, AZ, AC = "fsdp_0", "fsdp_1", "fsdp_2"
FSDP = (AX, AZ, AC)
SKEW = 2
GRANT = 14 << 20
TICK_GRANT = 6 << 20
CHUNK = 256
GRAD_CHUNK = 512
GELU_A = 0.7978845608028654
GELU_B = GELU_A * 0.044715
BF16, F32 = jnp.bfloat16, jnp.float32


ANY = pl.BlockSpec(memory_space=pl.ANY)
SMEM = pl.BlockSpec(memory_space=pltpu.SMEM)
VMEM = pl.BlockSpec(memory_space=pltpu.VMEM)


def shift(value, axis, distance, wrap=True):
    n = lax.axis_size(axis)
    if wrap:
        route = [(i, (i + distance) % n) for i in range(n)]
    else:
        route = [(i, i + distance) for i in range(n) if 0 <= i + distance < n]
    return lax.ppermute(value, axis, route)


def gather_pieces(own, first, second):
    line = jnp.stack([own] + [shift(own, first, -r) for r in (1, 2, 3)])
    ahead, behind = shift(line, second, -1), shift(line, second, 1)
    low = shift(behind[:2], second, 1)
    high = shift(ahead[2:], second, -1)
    mine = (line, ahead, behind, low, high)
    return mine + tuple(shift(p, AC, 1) for p in mine)


def placements(first_at, second_at, core):
    rows = []
    for own in (0, 1):
        c = core if own == 0 else 1 - core
        for piece, r2, r1s in ((0, 0, range(4)), (1, 1, range(4)), (2, 3, range(4)), (3, 2, (0, 1)), (4, 2, (2, 3))):
            for at, r1 in enumerate(r1s):
                rows.append((5 * own + piece, at, (first_at + r1) & 3, (second_at + r2) & 3, c))
    return rows


def assemble_kernel(place, *refs):
    ups, downs = refs[:10], refs[10:20]
    w_up, w_down, x_st, st_st, at_st, gp_st, g_st, gh_st, gg_st, sem_up, sem_down = refs[20:]
    x, z, c = place[0], place[1], place[2]
    n_up, n_down = w_up.shape[0] // 32, w_down.shape[0] // 32
    copies = []
    for piece, at, fx, fz, core in placements(x, z, c):
        rows = pl.ds(pl.multiple_of((fx * 8 + fz * 2 + core) * n_up, n_up), n_up)
        copies.append(pltpu.make_async_copy(ups[piece].at[at], w_up.at[rows], sem_up.at[len(copies)]))
    late = []
    for piece, at, fz, fx, core in placements(z, x, c):
        rows = pl.ds(pl.multiple_of((fx * 8 + fz * 2 + core) * n_down, n_down), n_down)
        late.append(pltpu.make_async_copy(downs[piece].at[at], w_down.at[rows], sem_down.at[len(late)]))
    for copy in copies + late:
        copy.start()
    for ref in (st_st, at_st, g_st, gh_st, gg_st):

        @pl.loop(0, ref.shape[0] // 64)
        def clear(i, ref=ref):
            ref[pl.ds(pl.multiple_of(i * 64, 64), 64), :] = jnp.zeros((64, ref.shape[1]), ref.dtype)

    for copy in copies + late:
        copy.wait()


def assemble(place, ups, downs, micros, rows):
    feat, hidden, tokens = 32 * ups[0].shape[1], ups[0].shape[2], micros * rows
    shapes = (
        (feat, hidden),
        (hidden, feat),
        (tokens, feat),
        (feat, tokens),
        (hidden, tokens),
        (tokens, hidden),
        (tokens, feat),
        (tokens, hidden),
    )
    return pl.pallas_call(
        assemble_kernel,
        out_shape=tuple(pltpu.VMEM(s, BF16) for s in shapes) + (pltpu.VMEM((8 * micros, feat), F32),),
        in_specs=[SMEM] + [ANY] * 20,
        out_specs=(VMEM,) * 9,
        scratch_shapes=[pltpu.SemaphoreType.DMA((32,)), pltpu.SemaphoreType.DMA((32,))],
        compiler_params=pltpu.CompilerParams(vmem_limit_bytes=GRANT),
        name="assemble",
    )(place, *ups, *downs)


def norm_of(values, mask, width):
    mean = jnp.sum(values, axis=-1, keepdims=True) / width
    centered = jnp.where(mask, values - mean, 0.0)
    variance = jnp.sum(centered * centered, axis=-1, keepdims=True) / width
    inv_std = lax.rsqrt(variance + EPSILON)
    return centered * inv_std, inv_std


def held(value):
    return pltpu.with_memory_space_constraint(value, pltpu.VMEM)


def cost_of(flops):
    return pl.CostEstimate(flops=flops, transcendentals=0, bytes_accessed=0)


def span(index, size):
    return pl.ds(pl.multiple_of(index * size, size), size)


def job_of(tab, q, micros):
    sec = tab[4 * micros]
    at = jnp.clip(q, 0, micros - 1)
    micro, width, hidden, depth = tab[at], tab[micros + at], tab[2 * micros + at], tab[3 * micros + at]
    valid = jnp.logical_and(jnp.logical_and(q >= 0, q < micros), depth > sec)
    return sec, at, micro, width, hidden, depth, valid


def forward_kernel(tab, patches, incoming, w_up, w_down, _x, _st, _at, _gp, *refs, tick):
    out, x_st, st_st, at_st, gp_st, normed, hid_buf, act_buf, acc = refs
    micros, rows, _ = patches.shape
    sec, at, micro, width, hidden, _, valid = job_of(tab, tick - SKEW * tab[4 * micros], micros)

    @pl.when(valid)
    def run():
        used = (hidden + CHUNK - 1) // CHUNK
        mine = span(at, rows)

        @pl.when(sec == 0)
        def first():
            acc[...] = patches[micro].astype(F32)

        @pl.when(sec != 0)
        def later():
            acc[...] = incoming[...].astype(F32)

        mask = lax.broadcasted_iota(jnp.int32, acc.shape, 1) < width
        values = jnp.where(mask, acc[...], 0.0)
        acc[...] = values
        x_st[mine, :] = values.astype(BF16)
        standard, _ = norm_of(values, mask, width.astype(F32))
        normed[...] = standard.astype(BF16)
        st_st[:, mine] = standard.T.astype(BF16)
        act_buf[...] = jnp.zeros(act_buf.shape, BF16)
        hid_buf[...] = jnp.dot(normed[...], w_up[:, :CHUNK], preferred_element_type=F32)

        @pl.loop(0, used)
        def step(c):
            h, ready = hid_buf[...], act_buf[...]
            following = jnp.minimum(c + 1, used - 1)
            hid_next = jnp.dot(normed[...], w_up[:, span(following, CHUNK)], preferred_element_type=F32)
            before = jnp.maximum(c - 1, 0)
            acc[...] += jnp.dot(ready, w_down[span(before, CHUNK), :], preferred_element_type=F32)
            h2 = h * h
            t = jnp.tanh(h * (GELU_A + GELU_B * h2))
            p = 0.5 + 0.5 * t
            act = h * p
            slope = p + act * (1.0 - t) * (GELU_A + (3.0 * GELU_B) * h2)
            inside = lax.broadcasted_iota(jnp.int32, h.shape, 1) < hidden - c * CHUNK
            act = jnp.where(inside, act, 0.0)
            act_buf[...] = act.astype(BF16)
            at_st[span(c, CHUNK), mine] = act.T.astype(BF16)
            gp_st[mine, span(c, CHUNK)] = jnp.where(inside, slope, 0.0).astype(BF16)
            hid_buf[...] = hid_next

        total = acc[...] + jnp.dot(act_buf[...], w_down[span(used - 1, CHUNK), :], preferred_element_type=F32)
        out[...] = jnp.where(mask, total, 0.0).astype(BF16)


def forward(tick, tab, patches, incoming, w_up, w_down, stash):
    _, rows, feat = patches.shape
    operands = [tab, held(patches), held(incoming), held(w_up), held(w_down)] + [held(s) for s in stash]
    out, *stash = pl.pallas_call(
        functools.partial(forward_kernel, tick=tick),
        out_shape=(jax.ShapeDtypeStruct((rows, feat), BF16),) + tuple(pltpu.VMEM(s.shape, s.dtype) for s in stash),
        in_specs=[SMEM] + [VMEM] * 8,
        out_specs=(VMEM,) * 5,
        scratch_shapes=[
            pltpu.VMEM((rows, feat), BF16),
            pltpu.VMEM((rows, CHUNK), F32),
            pltpu.VMEM((rows, CHUNK), BF16),
            pltpu.VMEM((rows, feat), F32),
        ],
        input_output_aliases={5 + k: 1 + k for k in range(4)},
        compiler_params=pltpu.CompilerParams(vmem_limit_bytes=TICK_GRANT),
        cost_estimate=cost_of(4 * rows * feat * w_up.shape[1]),
        name="forward",
    )(*operands)
    return out, tuple(stash)


def backward_kernel(tab, cotangent, incoming, w_up, w_down, x_st, gp_st, _at, _g, _gh, _gg, *refs, tick):
    out, g_st, gh_st, gg_st, g_buf, gh_buf, acc = refs
    micros, rows, _ = cotangent.shape
    q = (micros - 1) - (tick + SKEW * (tab[4 * micros] - 1))
    sec, at, micro, width, hidden, depth, valid = job_of(tab, q, micros)

    @pl.when(valid)
    def run():
        used = (hidden + CHUNK - 1) // CHUNK
        mine = span(at, rows)

        @pl.when(depth == sec + 1)
        def last():
            g_buf[...] = cotangent[micro]

        @pl.when(depth != sec + 1)
        def inner():
            g_buf[...] = incoming[...]

        mask = lax.broadcasted_iota(jnp.int32, acc.shape, 1) < width
        grad_branch = jnp.where(mask, g_buf[...].astype(F32), 0.0).astype(BF16)
        g_buf[...] = grad_branch
        g_st[mine, :] = grad_branch
        acc[...] = jnp.zeros(acc.shape, F32)
        gh_buf[...] = jnp.zeros(gh_buf.shape, BF16)
        nt = (((1,), (1,)), ((), ()))

        @pl.loop(0, used)
        def step(c):
            ready = gh_buf[...]
            grad_act = lax.dot_general(g_buf[...], w_down[span(c, CHUNK), :], nt, preferred_element_type=F32)
            before = jnp.maximum(c - 1, 0)
            acc[...] += lax.dot_general(ready, w_up[:, span(before, CHUNK)], nt, preferred_element_type=F32)
            grad_hid = (grad_act * gp_st[mine, span(c, CHUNK)].astype(F32)).astype(BF16)
            gh_buf[...] = grad_hid
            gh_st[mine, span(c, CHUNK)] = grad_hid

        total = acc[...] + lax.dot_general(
            gh_buf[...], w_up[:, span(used - 1, CHUNK)], nt, preferred_element_type=F32
        )
        width_float = width.astype(F32)
        standard, inv_std = norm_of(x_st[mine, :].astype(F32), mask, width_float)
        grad_std = jnp.where(mask, total, 0.0)
        product = grad_std * standard
        gg_st[span(at, 8), :] = jnp.sum(product.reshape(-1, 8, product.shape[1]), axis=0)
        first_mean = jnp.sum(grad_std, axis=-1, keepdims=True) / width_float
        second_mean = jnp.sum(product, axis=-1, keepdims=True) / width_float
        grad_in = inv_std * (grad_std - first_mean - standard * second_mean)
        out[...] = jnp.where(mask, g_buf[...].astype(F32) + grad_in, 0.0).astype(BF16)


def backward(tick, tab, cotangent, incoming, w_up, w_down, x_st, gp_st, at_st, stash):
    _, rows, feat = cotangent.shape
    operands = [tab] + [held(v) for v in (cotangent, incoming, w_up, w_down, x_st, gp_st, at_st) + tuple(stash)]
    out, *stash = pl.pallas_call(
        functools.partial(backward_kernel, tick=tick),
        out_shape=(jax.ShapeDtypeStruct((rows, feat), BF16),) + tuple(pltpu.VMEM(s.shape, s.dtype) for s in stash),
        in_specs=[SMEM] + [VMEM] * 10,
        out_specs=(VMEM,) * 4,
        scratch_shapes=[
            pltpu.VMEM((rows, feat), BF16),
            pltpu.VMEM((rows, CHUNK), BF16),
            pltpu.VMEM((rows, feat), F32),
        ],
        input_output_aliases={8 + k: 1 + k for k in range(3)},
        compiler_params=pltpu.CompilerParams(vmem_limit_bytes=TICK_GRANT),
        cost_estimate=cost_of(4 * rows * feat * w_up.shape[1]),
        name="backward",
    )(*operands)
    return out, tuple(stash)


def split_cores(core, blocks, mine, theirs, value_of):
    for parity, targets in ((0, (mine, theirs)), (1, (theirs, mine))):

        @pl.when(core == parity)
        def write(targets=targets):
            for f in range(blocks):
                targets[f & 1](f >> 3, (f >> 1) & 3, value_of(f))


def up_kernel(place, st, gh, gg, own, par):
    x, z, core = place[0], place[1], place[2]
    hidden = gh.shape[1]
    n = st.shape[0] // 32

    def put(ref, columns):
        def write(fx, fz, value):
            ref[(fx - x) & 3, (fz - z) & 3, :, columns] = value

        return write

    @pl.loop(0, hidden // GRAD_CHUNK)
    def step(c):
        columns = span(c, GRAD_CHUNK)
        up = jnp.dot(st[...], gh[:, columns], preferred_element_type=F32).astype(BF16)
        split_cores(core, 32, put(own, columns), put(par, columns), lambda f: up[f * n : (f + 1) * n])

    total = gg[...]
    total = jnp.concatenate([total, jnp.zeros((128 - total.shape[0], total.shape[1]), F32)], axis=0)
    column = total.T.astype(BF16)
    last = pl.ds(hidden, 128)
    split_cores(core, 32, put(own, last), put(par, last), lambda f: column[f * n : (f + 1) * n])


def up_grads(place, st_st, gh_st, gg_st):
    feat, hidden = st_st.shape[0], gh_st.shape[1]
    out = jax.ShapeDtypeStruct((4, 4, feat // 32, hidden + 128), BF16)
    return pl.pallas_call(
        up_kernel,
        out_shape=(out, out),
        in_specs=[SMEM] + [VMEM] * 3,
        out_specs=(VMEM, VMEM),
        compiler_params=pltpu.CompilerParams(vmem_limit_bytes=GRANT),
        cost_estimate=cost_of(2 * feat * hidden * gh_st.shape[0]),
        name="up_grads",
    )(place, held(st_st), held(gh_st), held(gg_st))


def down_kernel(place, at, g, own, par):
    x, z, core = place[0], place[1], place[2]
    n = at.shape[0] // 32

    @pl.loop(0, 4)
    def step(i):
        down = jnp.dot(at[span(i, 8 * n), :], g[...], preferred_element_type=F32).astype(BF16)
        for parity, targets in ((0, (own, par)), (1, (par, own))):

            @pl.when(core == parity)
            def write(targets=targets):
                for f in range(8):
                    targets[f & 1][((f >> 1) - z) & 3, (i - x) & 3] = down[f * n : (f + 1) * n]


def down_grads(place, at_st, g_st):
    out = jax.ShapeDtypeStruct((4, 4, at_st.shape[0] // 32, g_st.shape[1]), BF16)
    return pl.pallas_call(
        down_kernel,
        out_shape=(out, out),
        in_specs=[SMEM] + [VMEM] * 2,
        out_specs=(VMEM, VMEM),
        compiler_params=pltpu.CompilerParams(vmem_limit_bytes=GRANT),
        cost_estimate=cost_of(2 * g_st.shape[1] * at_st.shape[0] * at_st.shape[1]),
        name="down_grads",
    )(place, held(at_st), held(g_st))


def plus(*values):
    total = values[0].astype(F32)
    for v in values[1:]:
        total = total + v.astype(F32)
    return total


def scatter_sum(own, partner, first, second):
    other = shift(partner, AC, 1)

    def joined(*at):
        return plus(own[at], other[at])

    low = shift(joined(2, slice(0, 2)).astype(BF16), first, 1)
    high = shift(joined(2, slice(2, 4)).astype(BF16), first, -1)
    ahead = jnp.concatenate([plus(joined(1, slice(0, 2)), low), joined(1, slice(2, 4))]).astype(BF16)
    behind = jnp.concatenate([joined(3, slice(0, 2)), plus(joined(3, slice(2, 4)), high)]).astype(BF16)
    line = plus(joined(0), shift(ahead, first, 1), shift(behind, first, -1))
    parts = [shift(line[r].astype(BF16), second, r) for r in (1, 2, 3)]
    return plus(line[0], *parts)


def schedule_table(embed_blocks, ratio_index, depth):
    micros = depth.shape[0]
    index = lax.iota(jnp.int32, micros)
    before = jnp.logical_or(
        depth[None, :] > depth[:, None],
        jnp.logical_and(depth[None, :] == depth[:, None], index[None, :] < index[:, None]),
    )
    rank = jnp.sum(before.astype(jnp.int32), axis=1)
    chosen = rank[None, :] == index[:, None]
    width = embed_blocks * BLOCK
    hidden = width * (6 + ratio_index) // 2
    columns = jnp.stack([index, width, hidden, depth])
    table = jnp.sum(jnp.where(chosen[None], columns[:, None, :], 0), axis=2)
    section = lax.axis_index("section").astype(jnp.int32)
    return jnp.concatenate([table.reshape(-1), jnp.full((8,), section, jnp.int32)])


def window(extra, tab, place, gain, patches, cotangent, ups, downs):
    micros, rows, _ = patches.shape
    up, down, *stash, g_st, gh_st, gg_st = assemble(place, ups, downs, micros, rows)
    hidden = up.shape[1]
    main = micros + SKEW

    outs = []
    for t in range(main + extra):
        incoming = shift(outs[t - SKEW], "section", 1, wrap=False) if t >= SKEW else patches[0]
        out, stash = forward(t, tab, patches, incoming, up, down, stash)
        outs.append(out)
    x_st, st_st, at_st, gp_st = stash

    back = (g_st, gh_st, gg_st)
    outs = []
    for t in range(main + extra):
        incoming = shift(outs[t - SKEW], "section", -1, wrap=False) if t >= SKEW else cotangent[0]
        out, back = backward(t - extra, tab, cotangent, incoming, up, down, x_st, gp_st, at_st, back)
        outs.append(out)
    g_st, gh_st, gg_st = back

    down_own, down_par = down_grads(place, at_st, g_st)
    up_own, up_par = up_grads(place, st_st, gh_st, gg_st)
    down_sum = scatter_sum(down_own, down_par, AZ, AX)
    up_sum = scatter_sum(up_own, up_par, AX, AZ)
    grad_up = up_sum[:, :hidden] * gain
    grad_gain = jnp.sum(up_sum[:, hidden:], axis=1) / gain[:, 0]
    return grad_up, down_sum, grad_gain


def per_device(patches, cotangent, embed_blocks, ratio_index, depth, w_up, w_down, ln_gain):
    sections = lax.axis_size("section")
    micros = patches.shape[0]
    gain = ln_gain[0].astype(F32)[:, None]
    place = jnp.stack([lax.axis_index(a) for a in FSDP]).astype(jnp.int32)
    tab = schedule_table(embed_blocks, ratio_index, depth)
    scaled = (w_up[0].astype(F32) * gain).astype(BF16)
    ups = gather_pieces(scaled, AX, AZ)
    downs = gather_pieces(w_down[0], AZ, AX)

    is_deep = jnp.zeros((), bool)
    for s in range(2, sections):
        reach = jnp.sum((depth > s).astype(jnp.int32))
        is_deep = jnp.logical_or(is_deep, reach > micros - SKEW * (s - 1))
    results = lax.cond(
        is_deep,
        functools.partial(window, SKEW * (sections - 2)),
        functools.partial(window, 0),
        *(tab, place, gain, patches, cotangent, ups, downs),
    )
    return tuple(r[None] for r in results)


def solution(mesh):
    finer = Mesh(
        mesh.devices.reshape(mesh.shape["section"], 4, 4, 2),
        ("section",) + FSDP,
    )
    in_specs = (
        P(None, FSDP, None),
        P(None, FSDP, None),
        P(),
        P(),
        P(),
        P("section", FSDP, None),
        P("section", FSDP, None),
        P("section", FSDP),
    )
    out_specs = (P("section", FSDP, None), P("section", FSDP, None), P("section", FSDP))
    return jax.shard_map(
        per_device, mesh=finer, in_specs=in_specs, out_specs=out_specs, check_vma=False
    )
```

```python
import functools

import jax
import jax.numpy as jnp
from jax import lax
from jax.experimental import pallas as pl
from jax.experimental.pallas import tpu as pltpu
from jax.sharding import Mesh
from jax.sharding import PartitionSpec as P

BLOCK = 128
EPSILON = 1e-05
AX, AZ, AC = "fsdp_0", "fsdp_1", "fsdp_2"
FSDP = (AX, AZ, AC)
SKEW = 2
GRANT = 13 << 20
TICK_GRANT = 3 << 20
CHUNK = 256
GRAD_CHUNK = 512
GELU_A = 0.7978845608028654
GELU_B = GELU_A * 0.044715
BF16, F32 = jnp.bfloat16, jnp.float32


ANY = pl.BlockSpec(memory_space=pl.ANY)
SMEM = pl.BlockSpec(memory_space=pltpu.SMEM)
VMEM = pl.BlockSpec(memory_space=pltpu.VMEM)


def shift(value, axis, distance, wrap=True):
    n = lax.axis_size(axis)
    if wrap:
        route = [(i, (i + distance) % n) for i in range(n)]
    else:
        route = [(i, i + distance) for i in range(n) if 0 <= i + distance < n]
    return lax.ppermute(value, axis, route)


def gather_pieces(own, first, second):
    ahead, behind, across = shift(own, first, -1), shift(own, first, 1), shift(own, first, 2)
    low = jnp.stack([own, ahead])
    high = jnp.stack([across, behind])
    low_ahead, low_behind = shift(low, second, -1), shift(low, second, 1)
    high_ahead, high_behind = shift(high, second, -1), shift(high, second, 1)
    low_across = shift(low_behind, second, 1)
    high_across = shift(high_ahead, second, -1)
    mine = (low, high, low_ahead, high_ahead, low_behind, high_behind, low_across, high_across)
    return mine + tuple(shift(p, AC, 1) for p in mine)


PIECES = 16


def placements(first_at, second_at, core):
    rows = []
    for own in (0, 1):
        c = core if own == 0 else 1 - core
        for place, r2 in enumerate((0, 1, 3, 2)):
            for half in (0, 1):
                for at in (0, 1):
                    piece = PIECES // 2 * own + 2 * place + half
                    rows.append((piece, at, (first_at + 2 * half + at) & 3, (second_at + r2) & 3, c))
    return rows


def assemble_kernel(place, *refs):
    ups, downs = refs[:PIECES], refs[PIECES : 2 * PIECES]
    w_up, w_down, x_st, st_st, at_st, gp_st, g_st, gh_st, gg_st, sem_up, sem_down = refs[2 * PIECES :]
    x, z, c = place[0], place[1], place[2]
    n_up, n_down = w_up.shape[0] // 32, w_down.shape[0] // 32
    copies = []
    for piece, at, fx, fz, core in placements(x, z, c):
        rows = pl.ds(pl.multiple_of((fx * 8 + fz * 2 + core) * n_up, n_up), n_up)
        copies.append(pltpu.make_async_copy(ups[piece].at[at], w_up.at[rows], sem_up.at[len(copies)]))
    late = []
    for piece, at, fz, fx, core in placements(z, x, c):
        rows = pl.ds(pl.multiple_of((fx * 8 + fz * 2 + core) * n_down, n_down), n_down)
        late.append(pltpu.make_async_copy(downs[piece].at[at], w_down.at[rows], sem_down.at[len(late)]))
    for copy in copies + late:
        copy.start()
    for ref in (st_st, at_st, g_st, gh_st, gg_st):

        @pl.loop(0, ref.shape[0] // 64)
        def clear(i, ref=ref):
            ref[pl.ds(pl.multiple_of(i * 64, 64), 64), :] = jnp.zeros((64, ref.shape[1]), ref.dtype)

    for copy in copies + late:
        copy.wait()


def assemble(place, ups, downs, micros, rows):
    feat, hidden, tokens = 32 * ups[0].shape[1], ups[0].shape[2], micros * rows
    shapes = (
        (feat, hidden),
        (hidden, feat),
        (tokens, feat),
        (feat, tokens),
        (hidden, tokens),
        (tokens, hidden),
        (tokens, feat),
        (tokens, hidden),
    )
    return pl.pallas_call(
        assemble_kernel,
        out_shape=tuple(pltpu.VMEM(s, BF16) for s in shapes) + (pltpu.VMEM((8 * micros, feat), F32),),
        in_specs=[SMEM] + [ANY] * (2 * PIECES),
        out_specs=(VMEM,) * 9,
        scratch_shapes=[pltpu.SemaphoreType.DMA((32,)), pltpu.SemaphoreType.DMA((32,))],
        compiler_params=pltpu.CompilerParams(vmem_limit_bytes=GRANT),
        name="assemble",
    )(place, *ups, *downs)


def norm_of(values, mask, width):
    mean = jnp.sum(values, axis=-1, keepdims=True) / width
    centered = jnp.where(mask, values - mean, 0.0)
    variance = jnp.sum(centered * centered, axis=-1, keepdims=True) / width
    inv_std = lax.rsqrt(variance + EPSILON)
    return centered * inv_std, inv_std


def held(value):
    return pltpu.with_memory_space_constraint(value, pltpu.VMEM)


def cost_of(flops):
    return pl.CostEstimate(flops=flops, transcendentals=0, bytes_accessed=0)


def span(index, size):
    return pl.ds(pl.multiple_of(index * size, size), size)


def job_of(tab, q, micros):
    sec = tab[4 * micros]
    at = jnp.clip(q, 0, micros - 1)
    micro, width, hidden, depth = tab[at], tab[micros + at], tab[2 * micros + at], tab[3 * micros + at]
    valid = jnp.logical_and(jnp.logical_and(q >= 0, q < micros), depth > sec)
    return sec, at, micro, width, hidden, depth, valid


def forward_kernel(tab, patches, incoming, w_up, w_down, _x, _st, _at, _gp, *refs, tick):
    out, x_st, st_st, at_st, gp_st, normed, hid_buf, act_buf, acc = refs
    micros, rows, _ = patches.shape
    sec, at, micro, width, hidden, _, valid = job_of(tab, tick - SKEW * tab[4 * micros], micros)

    @pl.when(valid)
    def run():
        used = (hidden + CHUNK - 1) // CHUNK
        mine = span(at, rows)

        @pl.when(sec == 0)
        def first():
            acc[...] = patches[micro].astype(F32)

        @pl.when(sec != 0)
        def later():
            acc[...] = incoming[...].astype(F32)

        mask = lax.broadcasted_iota(jnp.int32, acc.shape, 1) < width
        values = jnp.where(mask, acc[...], 0.0)
        acc[...] = values
        x_st[mine, :] = values.astype(BF16)
        standard, _ = norm_of(values, mask, width.astype(F32))
        normed[...] = standard.astype(BF16)
        st_st[:, mine] = standard.T.astype(BF16)
        act_buf[...] = jnp.zeros(act_buf.shape, BF16)
        hid_buf[...] = jnp.dot(normed[...], w_up[:, :CHUNK], preferred_element_type=F32)

        @pl.loop(0, used)
        def step(c):
            h, ready = hid_buf[...], act_buf[...]
            following = jnp.minimum(c + 1, used - 1)
            hid_next = jnp.dot(normed[...], w_up[:, span(following, CHUNK)], preferred_element_type=F32)
            before = jnp.maximum(c - 1, 0)
            acc[...] += jnp.dot(ready, w_down[span(before, CHUNK), :], preferred_element_type=F32)
            h2 = h * h
            t = jnp.tanh(h * (GELU_A + GELU_B * h2))
            p = 0.5 + 0.5 * t
            act = h * p
            slope = p + act * (1.0 - t) * (GELU_A + (3.0 * GELU_B) * h2)
            inside = lax.broadcasted_iota(jnp.int32, h.shape, 1) < hidden - c * CHUNK
            act = jnp.where(inside, act, 0.0)
            act_buf[...] = act.astype(BF16)
            at_st[span(c, CHUNK), mine] = act.T.astype(BF16)
            gp_st[mine, span(c, CHUNK)] = jnp.where(inside, slope, 0.0).astype(BF16)
            hid_buf[...] = hid_next

        total = acc[...] + jnp.dot(act_buf[...], w_down[span(used - 1, CHUNK), :], preferred_element_type=F32)
        out[...] = jnp.where(mask, total, 0.0).astype(BF16)


def forward(tick, tab, patches, incoming, w_up, w_down, stash):
    _, rows, feat = patches.shape
    operands = [tab, held(patches), held(incoming), held(w_up), held(w_down)] + [held(s) for s in stash]
    out, *stash = pl.pallas_call(
        functools.partial(forward_kernel, tick=tick),
        out_shape=(jax.ShapeDtypeStruct((rows, feat), BF16),) + tuple(pltpu.VMEM(s.shape, s.dtype) for s in stash),
        in_specs=[SMEM] + [VMEM] * 8,
        out_specs=(VMEM,) * 5,
        scratch_shapes=[
            pltpu.VMEM((rows, feat), BF16),
            pltpu.VMEM((rows, CHUNK), F32),
            pltpu.VMEM((rows, CHUNK), BF16),
            pltpu.VMEM((rows, feat), F32),
        ],
        input_output_aliases={5 + k: 1 + k for k in range(4)},
        compiler_params=pltpu.CompilerParams(vmem_limit_bytes=TICK_GRANT),
        cost_estimate=cost_of(4 * rows * feat * w_up.shape[1]),
        name="forward",
    )(*operands)
    return out, tuple(stash)


def backward_kernel(tab, cotangent, incoming, w_up, w_down, x_st, gp_st, _at, _g, _gh, _gg, *refs, tick):
    out, g_st, gh_st, gg_st, g_buf, gh_buf, acc = refs
    micros, rows, _ = cotangent.shape
    q = (micros - 1) - (tick + SKEW * (tab[4 * micros] - 1))
    sec, at, micro, width, hidden, depth, valid = job_of(tab, q, micros)

    @pl.when(valid)
    def run():
        used = (hidden + CHUNK - 1) // CHUNK
        mine = span(at, rows)

        @pl.when(depth == sec + 1)
        def last():
            g_buf[...] = cotangent[micro]

        @pl.when(depth != sec + 1)
        def inner():
            g_buf[...] = incoming[...]

        mask = lax.broadcasted_iota(jnp.int32, acc.shape, 1) < width
        grad_branch = jnp.where(mask, g_buf[...].astype(F32), 0.0).astype(BF16)
        g_buf[...] = grad_branch
        g_st[mine, :] = grad_branch
        acc[...] = jnp.zeros(acc.shape, F32)
        gh_buf[...] = jnp.zeros(gh_buf.shape, BF16)
        nt = (((1,), (1,)), ((), ()))

        @pl.loop(0, used)
        def step(c):
            ready = gh_buf[...]
            grad_act = lax.dot_general(g_buf[...], w_down[span(c, CHUNK), :], nt, preferred_element_type=F32)
            before = jnp.maximum(c - 1, 0)
            acc[...] += lax.dot_general(ready, w_up[:, span(before, CHUNK)], nt, preferred_element_type=F32)
            grad_hid = (grad_act * gp_st[mine, span(c, CHUNK)].astype(F32)).astype(BF16)
            gh_buf[...] = grad_hid
            gh_st[mine, span(c, CHUNK)] = grad_hid

        total = acc[...] + lax.dot_general(
            gh_buf[...], w_up[:, span(used - 1, CHUNK)], nt, preferred_element_type=F32
        )
        width_float = width.astype(F32)
        standard, inv_std = norm_of(x_st[mine, :].astype(F32), mask, width_float)
        grad_std = jnp.where(mask, total, 0.0)
        product = grad_std * standard
        gg_st[span(at, 8), :] = jnp.sum(product.reshape(-1, 8, product.shape[1]), axis=0)
        first_mean = jnp.sum(grad_std, axis=-1, keepdims=True) / width_float
        second_mean = jnp.sum(product, axis=-1, keepdims=True) / width_float
        grad_in = inv_std * (grad_std - first_mean - standard * second_mean)
        out[...] = jnp.where(mask, g_buf[...].astype(F32) + grad_in, 0.0).astype(BF16)


def backward(tick, tab, cotangent, incoming, w_up, w_down, x_st, gp_st, at_st, stash):
    _, rows, feat = cotangent.shape
    operands = [tab] + [held(v) for v in (cotangent, incoming, w_up, w_down, x_st, gp_st, at_st) + tuple(stash)]
    out, *stash = pl.pallas_call(
        functools.partial(backward_kernel, tick=tick),
        out_shape=(jax.ShapeDtypeStruct((rows, feat), BF16),) + tuple(pltpu.VMEM(s.shape, s.dtype) for s in stash),
        in_specs=[SMEM] + [VMEM] * 10,
        out_specs=(VMEM,) * 4,
        scratch_shapes=[
            pltpu.VMEM((rows, feat), BF16),
            pltpu.VMEM((rows, CHUNK), BF16),
            pltpu.VMEM((rows, feat), F32),
        ],
        input_output_aliases={8 + k: 1 + k for k in range(3)},
        compiler_params=pltpu.CompilerParams(vmem_limit_bytes=TICK_GRANT),
        cost_estimate=cost_of(4 * rows * feat * w_up.shape[1]),
        name="backward",
    )(*operands)
    return out, tuple(stash)


def split_cores(core, blocks, mine, theirs, value_of):
    for parity, targets in ((0, (mine, theirs)), (1, (theirs, mine))):

        @pl.when(core == parity)
        def write(targets=targets):
            for f in range(blocks):
                targets[f & 1](f >> 3, (f >> 1) & 3, value_of(f))


def up_kernel(place, st, gh, gg, own, par):
    x, z, core = place[0], place[1], place[2]
    hidden = gh.shape[1]
    n = st.shape[0] // 32

    def put(ref, columns):
        def write(fx, fz, value):
            ref[(fx - x) & 3, (fz - z) & 3, :, columns] = value

        return write

    @pl.loop(0, hidden // GRAD_CHUNK)
    def step(c):
        columns = span(c, GRAD_CHUNK)
        up = jnp.dot(st[...], gh[:, columns], preferred_element_type=F32).astype(BF16)
        split_cores(core, 32, put(own, columns), put(par, columns), lambda f: up[f * n : (f + 1) * n])

    total = gg[...]
    total = jnp.concatenate([total, jnp.zeros((128 - total.shape[0], total.shape[1]), F32)], axis=0)
    column = total.T.astype(BF16)
    last = pl.ds(hidden, 128)
    split_cores(core, 32, put(own, last), put(par, last), lambda f: column[f * n : (f + 1) * n])


def up_grads(place, st_st, gh_st, gg_st):
    feat, hidden = st_st.shape[0], gh_st.shape[1]
    out = jax.ShapeDtypeStruct((4, 4, feat // 32, hidden + 128), BF16)
    return pl.pallas_call(
        up_kernel,
        out_shape=(out, out),
        in_specs=[SMEM] + [VMEM] * 3,
        out_specs=(VMEM, VMEM),
        compiler_params=pltpu.CompilerParams(vmem_limit_bytes=GRANT),
        cost_estimate=cost_of(2 * feat * hidden * gh_st.shape[0]),
        name="up_grads",
    )(place, held(st_st), held(gh_st), held(gg_st))


def down_kernel(place, at, g, own, par):
    x, z, core = place[0], place[1], place[2]
    n = at.shape[0] // 32

    @pl.loop(0, 4)
    def step(i):
        down = jnp.dot(at[span(i, 8 * n), :], g[...], preferred_element_type=F32).astype(BF16)
        for parity, targets in ((0, (own, par)), (1, (par, own))):

            @pl.when(core == parity)
            def write(targets=targets):
                for f in range(8):
                    targets[f & 1][((f >> 1) - z) & 3, (i - x) & 3] = down[f * n : (f + 1) * n]


def down_grads(place, at_st, g_st):
    out = jax.ShapeDtypeStruct((4, 4, at_st.shape[0] // 32, g_st.shape[1]), BF16)
    return pl.pallas_call(
        down_kernel,
        out_shape=(out, out),
        in_specs=[SMEM] + [VMEM] * 2,
        out_specs=(VMEM, VMEM),
        compiler_params=pltpu.CompilerParams(vmem_limit_bytes=GRANT),
        cost_estimate=cost_of(2 * g_st.shape[1] * at_st.shape[0] * at_st.shape[1]),
        name="down_grads",
    )(place, held(at_st), held(g_st))


def plus(*values):
    total = values[0].astype(F32)
    for v in values[1:]:
        total = total + v.astype(F32)
    return total


def scatter_sum(own, partner, first, second):
    other = shift(partner, AC, 1)

    def joined(*at):
        return plus(own[at], other[at])

    low = shift(joined(2, slice(0, 2)).astype(BF16), first, 1)
    high = shift(joined(2, slice(2, 4)).astype(BF16), first, -1)
    ahead = jnp.concatenate([plus(joined(1, slice(0, 2)), low), joined(1, slice(2, 4))]).astype(BF16)
    behind = jnp.concatenate([joined(3, slice(0, 2)), plus(joined(3, slice(2, 4)), high)]).astype(BF16)
    line = plus(joined(0), shift(ahead, first, 1), shift(behind, first, -1))
    parts = [shift(line[r].astype(BF16), second, r) for r in (1, 2, 3)]
    return plus(line[0], *parts)


def schedule_table(embed_blocks, ratio_index, depth):
    micros = depth.shape[0]
    index = lax.iota(jnp.int32, micros)
    before = jnp.logical_or(
        depth[None, :] > depth[:, None],
        jnp.logical_and(depth[None, :] == depth[:, None], index[None, :] < index[:, None]),
    )
    rank = jnp.sum(before.astype(jnp.int32), axis=1)
    chosen = rank[None, :] == index[:, None]
    width = embed_blocks * BLOCK
    hidden = width * (6 + ratio_index) // 2
    columns = jnp.stack([index, width, hidden, depth])
    table = jnp.sum(jnp.where(chosen[None], columns[:, None, :], 0), axis=2)
    section = lax.axis_index("section").astype(jnp.int32)
    return jnp.concatenate([table.reshape(-1), jnp.full((8,), section, jnp.int32)])


def window(extra, tab, place, gain, patches, cotangent, ups, downs):
    micros, rows, _ = patches.shape
    up, down, *stash, g_st, gh_st, gg_st = assemble(place, ups, downs, micros, rows)
    hidden = up.shape[1]
    main = micros + SKEW

    outs = []
    for t in range(main + extra):
        incoming = shift(outs[t - SKEW], "section", 1, wrap=False) if t >= SKEW else patches[0]
        out, stash = forward(t, tab, patches, incoming, up, down, stash)
        outs.append(out)
    x_st, st_st, at_st, gp_st = stash

    back = (g_st, gh_st, gg_st)
    outs = []
    for t in range(main + extra):
        incoming = shift(outs[t - SKEW], "section", -1, wrap=False) if t >= SKEW else cotangent[0]
        out, back = backward(t - extra, tab, cotangent, incoming, up, down, x_st, gp_st, at_st, back)
        outs.append(out)
    g_st, gh_st, gg_st = back

    down_own, down_par = down_grads(place, at_st, g_st)
    up_own, up_par = up_grads(place, st_st, gh_st, gg_st)
    down_sum = scatter_sum(down_own, down_par, AZ, AX)
    up_sum = scatter_sum(up_own, up_par, AX, AZ)
    grad_up = up_sum[:, :hidden] * gain
    grad_gain = jnp.sum(up_sum[:, hidden:], axis=1) / gain[:, 0]
    return grad_up, down_sum, grad_gain


def per_device(patches, cotangent, embed_blocks, ratio_index, depth, w_up, w_down, ln_gain):
    sections = lax.axis_size("section")
    micros = patches.shape[0]
    gain = ln_gain[0].astype(F32)[:, None]
    place = jnp.stack([lax.axis_index(a) for a in FSDP]).astype(jnp.int32)
    tab = schedule_table(embed_blocks, ratio_index, depth)
    scaled = (w_up[0].astype(F32) * gain).astype(BF16)
    ups = gather_pieces(scaled, AX, AZ)
    downs = gather_pieces(w_down[0], AZ, AX)

    extra = jnp.zeros((), jnp.int32)
    for s in range(2, sections):
        reach = jnp.sum((depth > s).astype(jnp.int32))
        extra = jnp.maximum(extra, reach - (micros - SKEW * (s - 1)))
    choices = (0, 1, SKEW * (sections - 2))
    branch = (extra > choices[0]).astype(jnp.int32) + (extra > choices[1]).astype(jnp.int32)
    results = lax.switch(
        branch,
        [functools.partial(window, n) for n in choices],
        *(tab, place, gain, patches, cotangent, ups, downs),
    )
    return tuple(r[None] for r in results)


def solution(mesh):
    finer = Mesh(
        mesh.devices.reshape(mesh.shape["section"], 4, 4, 2),
        ("section",) + FSDP,
    )
    in_specs = (
        P(None, FSDP, None),
        P(None, FSDP, None),
        P(),
        P(),
        P(),
        P("section", FSDP, None),
        P("section", FSDP, None),
        P("section", FSDP),
    )
    out_specs = (P("section", FSDP, None), P("section", FSDP, None), P("section", FSDP))
    return jax.shard_map(
        per_device, mesh=finer, in_specs=in_specs, out_specs=out_specs, check_vma=False
    )
```

```python
import functools

import jax
import jax.numpy as jnp
from jax import lax
from jax.experimental import pallas as pl
from jax.experimental.pallas import tpu as pltpu
from jax.sharding import Mesh
from jax.sharding import PartitionSpec as P

BLOCK = 128
EPSILON = 1e-05
AX, AZ, AC = "fsdp_0", "fsdp_1", "fsdp_2"
FSDP = (AX, AZ, AC)
SKEW = 2
GRANT = 13 << 20
TICK_GRANT = 3 << 20
CHUNK = 256
GRAD_CHUNK = 512
GELU_A = 0.7978845608028654
GELU_B = GELU_A * 0.044715
BF16, F32 = jnp.bfloat16, jnp.float32


ANY = pl.BlockSpec(memory_space=pl.ANY)
SMEM = pl.BlockSpec(memory_space=pltpu.SMEM)
VMEM = pl.BlockSpec(memory_space=pltpu.VMEM)


def shift(value, axis, distance, wrap=True):
    n = lax.axis_size(axis)
    if wrap:
        route = [(i, (i + distance) % n) for i in range(n)]
    else:
        route = [(i, i + distance) for i in range(n) if 0 <= i + distance < n]
    return lax.ppermute(value, axis, route)


def gather_pieces(own, first, second):
    ahead, behind, across = shift(own, first, -1), shift(own, first, 1), shift(own, first, 2)
    low = jnp.stack([own, ahead])
    high = jnp.stack([across, behind])
    low_ahead, low_behind = shift(low, second, -1), shift(low, second, 1)
    high_ahead, high_behind = shift(high, second, -1), shift(high, second, 1)
    low_across = shift(low_behind, second, 1)
    high_across = shift(high_ahead, second, -1)
    mine = (low, high, low_ahead, high_ahead, low_behind, high_behind, low_across, high_across)
    return mine + tuple(shift(p, AC, 1) for p in mine)


PIECES = 16


def placements(first_at, second_at, core):
    rows = []
    for own in (0, 1):
        c = core if own == 0 else 1 - core
        for place, r2 in enumerate((0, 1, 3, 2)):
            for half in (0, 1):
                for at in (0, 1):
                    piece = PIECES // 2 * own + 2 * place + half
                    rows.append((piece, at, (first_at + 2 * half + at) & 3, (second_at + r2) & 3, c))
    return rows


def assemble_kernel(place, *refs):
    ups, downs = refs[:PIECES], refs[PIECES : 2 * PIECES]
    w_up, w_down, x_st, st_st, at_st, gp_st, g_st, gh_st, _, gg_st, sem_up, sem_down = refs[2 * PIECES :]
    x, z, c = place[0], place[1], place[2]
    n_up, n_down = w_up.shape[0] // 32, w_down.shape[0] // 32
    copies = []
    for piece, at, fx, fz, core in placements(x, z, c):
        rows = pl.ds(pl.multiple_of((fx * 8 + fz * 2 + core) * n_up, n_up), n_up)
        copies.append(pltpu.make_async_copy(ups[piece].at[at], w_up.at[rows], sem_up.at[len(copies)]))
    late = []
    for piece, at, fz, fx, core in placements(z, x, c):
        rows = pl.ds(pl.multiple_of((fx * 8 + fz * 2 + core) * n_down, n_down), n_down)
        late.append(pltpu.make_async_copy(downs[piece].at[at], w_down.at[rows], sem_down.at[len(late)]))
    for copy in copies + late:
        copy.start()
    for ref in (st_st, at_st, g_st, gh_st, gg_st):

        @pl.loop(0, ref.shape[0] // 64)
        def clear(i, ref=ref):
            ref[pl.ds(pl.multiple_of(i * 64, 64), 64), :] = jnp.zeros((64, ref.shape[1]), ref.dtype)

    for copy in copies + late:
        copy.wait()


def assemble(place, ups, downs, micros, rows):
    feat, hidden, tokens = 32 * ups[0].shape[1], ups[0].shape[2], micros * rows
    shapes = (
        (feat, hidden),
        (hidden, feat),
        (tokens, feat),
        (feat, tokens),
        (hidden, tokens),
        (tokens, hidden),
        (tokens, feat),
        (tokens, hidden),
        (rows, feat),
    )
    return pl.pallas_call(
        assemble_kernel,
        out_shape=tuple(pltpu.VMEM(s, BF16) for s in shapes) + (pltpu.VMEM((8 * micros, feat), F32),),
        in_specs=[SMEM] + [ANY] * (2 * PIECES),
        out_specs=(VMEM,) * 10,
        scratch_shapes=[pltpu.SemaphoreType.DMA((32,)), pltpu.SemaphoreType.DMA((32,))],
        compiler_params=pltpu.CompilerParams(vmem_limit_bytes=GRANT),
        name="assemble",
    )(place, *ups, *downs)


def norm_of(values, mask, width):
    mean = jnp.sum(values, axis=-1, keepdims=True) / width
    centered = jnp.where(mask, values - mean, 0.0)
    variance = jnp.sum(centered * centered, axis=-1, keepdims=True) / width
    inv_std = lax.rsqrt(variance + EPSILON)
    return centered * inv_std, inv_std


def held(value):
    return pltpu.with_memory_space_constraint(value, pltpu.VMEM)


def cost_of(flops):
    return pl.CostEstimate(flops=flops, transcendentals=0, bytes_accessed=0)


def span(index, size):
    return pl.ds(pl.multiple_of(index * size, size), size)


def job_of(tab, q, micros):
    sec = tab[4 * micros]
    at = jnp.clip(q, 0, micros - 1)
    micro, width, hidden, depth = tab[at], tab[micros + at], tab[2 * micros + at], tab[3 * micros + at]
    valid = jnp.logical_and(jnp.logical_and(q >= 0, q < micros), depth > sec)
    return sec, at, micro, width, hidden, depth, valid


def forward_kernel(tab, patches, incoming, w_up, w_down, _x, _st, _at, _gp, *refs, tick):
    out, x_st, st_st, at_st, gp_st, normed, hid_buf, act_buf, acc = refs
    micros, rows, _ = patches.shape
    sec, at, micro, width, hidden, _, valid = job_of(tab, tick - SKEW * tab[4 * micros], micros)

    @pl.when(valid)
    def run():
        used = (hidden + CHUNK - 1) // CHUNK
        mine = span(at, rows)

        @pl.when(sec == 0)
        def first():
            acc[...] = patches[micro].astype(F32)

        @pl.when(sec != 0)
        def later():
            acc[...] = incoming[...].astype(F32)

        mask = lax.broadcasted_iota(jnp.int32, acc.shape, 1) < width
        values = jnp.where(mask, acc[...], 0.0)
        acc[...] = values
        x_st[mine, :] = values.astype(BF16)
        standard, _ = norm_of(values, mask, width.astype(F32))
        normed[...] = standard.astype(BF16)
        st_st[:, mine] = standard.T.astype(BF16)
        act_buf[...] = jnp.zeros(act_buf.shape, BF16)
        hid_buf[...] = jnp.dot(normed[...], w_up[:, :CHUNK], preferred_element_type=F32)

        @pl.loop(0, used)
        def step(c):
            h, ready = hid_buf[...], act_buf[...]
            following = jnp.minimum(c + 1, used - 1)
            hid_next = jnp.dot(normed[...], w_up[:, span(following, CHUNK)], preferred_element_type=F32)
            before = jnp.maximum(c - 1, 0)
            acc[...] += jnp.dot(ready, w_down[span(before, CHUNK), :], preferred_element_type=F32)
            h2 = h * h
            t = jnp.tanh(h * (GELU_A + GELU_B * h2))
            p = 0.5 + 0.5 * t
            act = h * p
            slope = p + act * (1.0 - t) * (GELU_A + (3.0 * GELU_B) * h2)
            inside = lax.broadcasted_iota(jnp.int32, h.shape, 1) < hidden - c * CHUNK
            act = jnp.where(inside, act, 0.0)
            act_buf[...] = act.astype(BF16)
            at_st[span(c, CHUNK), mine] = act.T.astype(BF16)
            gp_st[mine, span(c, CHUNK)] = jnp.where(inside, slope, 0.0).astype(BF16)
            hid_buf[...] = hid_next

        total = acc[...] + jnp.dot(act_buf[...], w_down[span(used - 1, CHUNK), :], preferred_element_type=F32)
        out[...] = jnp.where(mask, total, 0.0).astype(BF16)


def forward(tick, tab, patches, incoming, w_up, w_down, stash):
    _, rows, feat = patches.shape
    operands = [tab, held(patches), held(incoming), held(w_up), held(w_down)] + [held(s) for s in stash]
    out, *stash = pl.pallas_call(
        functools.partial(forward_kernel, tick=tick),
        out_shape=(jax.ShapeDtypeStruct((rows, feat), BF16),) + tuple(pltpu.VMEM(s.shape, s.dtype) for s in stash),
        in_specs=[SMEM] + [VMEM] * 8,
        out_specs=(VMEM,) * 5,
        scratch_shapes=[
            pltpu.VMEM((rows, feat), BF16),
            pltpu.VMEM((rows, CHUNK), F32),
            pltpu.VMEM((rows, CHUNK), BF16),
            pltpu.VMEM((rows, feat), F32),
        ],
        input_output_aliases={5 + k: 1 + k for k in range(4)},
        compiler_params=pltpu.CompilerParams(vmem_limit_bytes=TICK_GRANT),
        cost_estimate=cost_of(4 * rows * feat * w_up.shape[1]),
        name="forward",
    )(*operands)
    return out, tuple(stash)


def backward_kernel(tab, cotangent, incoming, w_up, w_down, x_st, gp_st, _at, _g, _gh, _gg, *refs, tick):
    out, g_st, gh_st, gg_st, g_buf, gh_buf, acc = refs
    micros, rows, _ = cotangent.shape
    q = (micros - 1) - (tick + SKEW * (tab[4 * micros] - 1))
    sec, at, micro, width, hidden, depth, valid = job_of(tab, q, micros)

    @pl.when(valid)
    def run():
        used = (hidden + CHUNK - 1) // CHUNK
        mine = span(at, rows)

        @pl.when(depth == sec + 1)
        def last():
            g_buf[...] = cotangent[micro]

        @pl.when(depth != sec + 1)
        def inner():
            g_buf[...] = incoming[...]

        mask = lax.broadcasted_iota(jnp.int32, acc.shape, 1) < width
        grad_branch = jnp.where(mask, g_buf[...].astype(F32), 0.0).astype(BF16)
        g_buf[...] = grad_branch
        g_st[mine, :] = grad_branch
        acc[...] = jnp.zeros(acc.shape, F32)
        gh_buf[...] = jnp.zeros(gh_buf.shape, BF16)
        nt = (((1,), (1,)), ((), ()))

        @pl.loop(0, used)
        def step(c):
            ready = gh_buf[...]
            grad_act = lax.dot_general(g_buf[...], w_down[span(c, CHUNK), :], nt, preferred_element_type=F32)
            before = jnp.maximum(c - 1, 0)
            acc[...] += lax.dot_general(ready, w_up[:, span(before, CHUNK)], nt, preferred_element_type=F32)
            grad_hid = (grad_act * gp_st[mine, span(c, CHUNK)].astype(F32)).astype(BF16)
            gh_buf[...] = grad_hid
            gh_st[mine, span(c, CHUNK)] = grad_hid

        total = acc[...] + lax.dot_general(
            gh_buf[...], w_up[:, span(used - 1, CHUNK)], nt, preferred_element_type=F32
        )
        width_float = width.astype(F32)
        standard, inv_std = norm_of(x_st[mine, :].astype(F32), mask, width_float)
        grad_std = jnp.where(mask, total, 0.0)
        product = grad_std * standard
        gg_st[span(at, 8), :] = jnp.sum(product.reshape(-1, 8, product.shape[1]), axis=0)
        first_mean = jnp.sum(grad_std, axis=-1, keepdims=True) / width_float
        second_mean = jnp.sum(product, axis=-1, keepdims=True) / width_float
        grad_in = inv_std * (grad_std - first_mean - standard * second_mean)
        out[...] = jnp.where(mask, g_buf[...].astype(F32) + grad_in, 0.0).astype(BF16)


def backward(tick, tab, cotangent, incoming, w_up, w_down, x_st, gp_st, at_st, stash):
    _, rows, feat = cotangent.shape
    operands = [tab] + [held(v) for v in (cotangent, incoming, w_up, w_down, x_st, gp_st, at_st) + tuple(stash)]
    out, *stash = pl.pallas_call(
        functools.partial(backward_kernel, tick=tick),
        out_shape=(jax.ShapeDtypeStruct((rows, feat), BF16),) + tuple(pltpu.VMEM(s.shape, s.dtype) for s in stash),
        in_specs=[SMEM] + [VMEM] * 10,
        out_specs=(VMEM,) * 4,
        scratch_shapes=[
            pltpu.VMEM((rows, feat), BF16),
            pltpu.VMEM((rows, CHUNK), BF16),
            pltpu.VMEM((rows, feat), F32),
        ],
        input_output_aliases={8 + k: 1 + k for k in range(3)},
        compiler_params=pltpu.CompilerParams(vmem_limit_bytes=TICK_GRANT),
        cost_estimate=cost_of(4 * rows * feat * w_up.shape[1]),
        name="backward",
    )(*operands)
    return out, tuple(stash)


def split_cores(core, blocks, mine, theirs, value_of):
    for parity, targets in ((0, (mine, theirs)), (1, (theirs, mine))):

        @pl.when(core == parity)
        def write(targets=targets):
            for f in range(blocks):
                targets[f & 1](f >> 3, (f >> 1) & 3, value_of(f))


def up_kernel(place, st, gh, gg, own, par):
    x, z, core = place[0], place[1], place[2]
    hidden = gh.shape[1]
    n = st.shape[0] // 32

    def put(ref, columns):
        def write(fx, fz, value):
            ref[(fx - x) & 3, (fz - z) & 3, :, columns] = value

        return write

    @pl.loop(0, hidden // GRAD_CHUNK)
    def step(c):
        columns = span(c, GRAD_CHUNK)
        up = jnp.dot(st[...], gh[:, columns], preferred_element_type=F32).astype(BF16)
        split_cores(core, 32, put(own, columns), put(par, columns), lambda f: up[f * n : (f + 1) * n])

    total = gg[...]
    total = jnp.concatenate([total, jnp.zeros((128 - total.shape[0], total.shape[1]), F32)], axis=0)
    column = total.T.astype(BF16)
    last = pl.ds(hidden, 128)
    split_cores(core, 32, put(own, last), put(par, last), lambda f: column[f * n : (f + 1) * n])


def up_grads(place, st_st, gh_st, gg_st):
    feat, hidden = st_st.shape[0], gh_st.shape[1]
    out = jax.ShapeDtypeStruct((4, 4, feat // 32, hidden + 128), BF16)
    return pl.pallas_call(
        up_kernel,
        out_shape=(out, out),
        in_specs=[SMEM] + [VMEM] * 3,
        out_specs=(VMEM, VMEM),
        compiler_params=pltpu.CompilerParams(vmem_limit_bytes=GRANT),
        cost_estimate=cost_of(2 * feat * hidden * gh_st.shape[0]),
        name="up_grads",
    )(place, held(st_st), held(gh_st), held(gg_st))


def down_kernel(place, at, g, own, par):
    x, z, core = place[0], place[1], place[2]
    n = at.shape[0] // 32

    @pl.loop(0, 4)
    def step(i):
        down = jnp.dot(at[span(i, 8 * n), :], g[...], preferred_element_type=F32).astype(BF16)
        for parity, targets in ((0, (own, par)), (1, (par, own))):

            @pl.when(core == parity)
            def write(targets=targets):
                for f in range(8):
                    targets[f & 1][((f >> 1) - z) & 3, (i - x) & 3] = down[f * n : (f + 1) * n]


def down_grads(place, at_st, g_st):
    out = jax.ShapeDtypeStruct((4, 4, at_st.shape[0] // 32, g_st.shape[1]), BF16)
    return pl.pallas_call(
        down_kernel,
        out_shape=(out, out),
        in_specs=[SMEM] + [VMEM] * 2,
        out_specs=(VMEM, VMEM),
        compiler_params=pltpu.CompilerParams(vmem_limit_bytes=GRANT),
        cost_estimate=cost_of(2 * g_st.shape[1] * at_st.shape[0] * at_st.shape[1]),
        name="down_grads",
    )(place, held(at_st), held(g_st))


def plus(*values):
    total = values[0].astype(F32)
    for v in values[1:]:
        total = total + v.astype(F32)
    return total


def scatter_sum(own, partner, first, second):
    other = shift(partner, AC, 1)

    def joined(*at):
        return plus(own[at], other[at])

    low = shift(joined(2, slice(0, 2)).astype(BF16), first, 1)
    high = shift(joined(2, slice(2, 4)).astype(BF16), first, -1)
    ahead = jnp.concatenate([plus(joined(1, slice(0, 2)), low), joined(1, slice(2, 4))]).astype(BF16)
    behind = jnp.concatenate([joined(3, slice(0, 2)), plus(joined(3, slice(2, 4)), high)]).astype(BF16)
    line = plus(joined(0), shift(ahead, first, 1), shift(behind, first, -1))
    parts = [shift(line[r].astype(BF16), second, r) for r in (1, 2, 3)]
    return plus(line[0], *parts)


def schedule_table(embed_blocks, ratio_index, depth):
    micros = depth.shape[0]
    index = lax.iota(jnp.int32, micros)
    before = jnp.logical_or(
        depth[None, :] > depth[:, None],
        jnp.logical_and(depth[None, :] == depth[:, None], index[None, :] < index[:, None]),
    )
    rank = jnp.sum(before.astype(jnp.int32), axis=1)
    chosen = rank[None, :] == index[:, None]
    width = embed_blocks * BLOCK
    hidden = width * (6 + ratio_index) // 2
    columns = jnp.stack([index, width, hidden, depth])
    table = jnp.sum(jnp.where(chosen[None], columns[:, None, :], 0), axis=2)
    section = lax.axis_index("section").astype(jnp.int32)
    return jnp.concatenate([table.reshape(-1), jnp.full((8,), section, jnp.int32)])


def window(extra, tab, place, gain, patches, cotangent, ups, downs):
    micros, rows, _ = patches.shape
    up, down, *stash, g_st, gh_st, unread, gg_st = assemble(place, ups, downs, micros, rows)
    hidden = up.shape[1]
    main = micros + SKEW

    outs = []
    for t in range(main + extra):
        incoming = shift(outs[t - SKEW], "section", 1, wrap=False) if t >= SKEW else unread
        out, stash = forward(t, tab, patches, incoming, up, down, stash)
        outs.append(out)
    x_st, st_st, at_st, gp_st = stash

    back = (g_st, gh_st, gg_st)
    outs = []
    for t in range(main + extra):
        incoming = shift(outs[t - SKEW], "section", -1, wrap=False) if t >= SKEW else unread
        out, back = backward(t - extra, tab, cotangent, incoming, up, down, x_st, gp_st, at_st, back)
        outs.append(out)
    g_st, gh_st, gg_st = back

    down_own, down_par = down_grads(place, at_st, g_st)
    up_own, up_par = up_grads(place, st_st, gh_st, gg_st)
    down_sum = scatter_sum(down_own, down_par, AZ, AX)
    up_sum = scatter_sum(up_own, up_par, AX, AZ)
    grad_up = up_sum[:, :hidden] * gain
    grad_gain = jnp.sum(up_sum[:, hidden:], axis=1) / gain[:, 0]
    return grad_up, down_sum, grad_gain


def per_device(patches, cotangent, embed_blocks, ratio_index, depth, w_up, w_down, ln_gain):
    sections = lax.axis_size("section")
    micros = patches.shape[0]
    gain = ln_gain[0].astype(F32)[:, None]
    place = jnp.stack([lax.axis_index(a) for a in FSDP]).astype(jnp.int32)
    tab = schedule_table(embed_blocks, ratio_index, depth)
    scaled = (w_up[0].astype(F32) * gain).astype(BF16)
    ups = gather_pieces(scaled, AX, AZ)
    downs = gather_pieces(w_down[0], AZ, AX)

    extra = jnp.zeros((), jnp.int32)
    for s in range(2, sections):
        reach = jnp.sum((depth > s).astype(jnp.int32))
        extra = jnp.maximum(extra, reach - (micros - SKEW * (s - 1)))
    choices = (0, 1, SKEW * (sections - 2))
    branch = (extra > choices[0]).astype(jnp.int32) + (extra > choices[1]).astype(jnp.int32)
    results = lax.switch(
        branch,
        [functools.partial(window, n) for n in choices],
        *(tab, place, gain, patches, cotangent, ups, downs),
    )
    return tuple(r[None] for r in results)


def solution(mesh):
    finer = Mesh(
        mesh.devices.reshape(mesh.shape["section"], 4, 4, 2),
        ("section",) + FSDP,
    )
    in_specs = (
        P(None, FSDP, None),
        P(None, FSDP, None),
        P(),
        P(),
        P(),
        P("section", FSDP, None),
        P("section", FSDP, None),
        P("section", FSDP),
    )
    out_specs = (P("section", FSDP, None), P("section", FSDP, None), P("section", FSDP))
    return jax.shard_map(
        per_device, mesh=finer, in_specs=in_specs, out_specs=out_specs, check_vma=False
    )
```

```python
import functools

import jax
import jax.numpy as jnp
from jax import lax
from jax.experimental import pallas as pl
from jax.experimental.pallas import tpu as pltpu
from jax.sharding import Mesh
from jax.sharding import PartitionSpec as P

BLOCK = 128
EPSILON = 1e-05
AX, AZ, AC = "fsdp_0", "fsdp_1", "fsdp_2"
FSDP = (AX, AZ, AC)
SKEW = 2
GRANT = 13 << 20
TICK_GRANT = 3 << 20
CHUNK = 256
GRAD_CHUNK = 512
GELU_A = 0.7978845608028654
GELU_B = GELU_A * 0.044715
BF16, F32 = jnp.bfloat16, jnp.float32


ANY = pl.BlockSpec(memory_space=pl.ANY)
SMEM = pl.BlockSpec(memory_space=pltpu.SMEM)
VMEM = pl.BlockSpec(memory_space=pltpu.VMEM)


def shift(value, axis, distance, wrap=True):
    n = lax.axis_size(axis)
    if wrap:
        route = [(i, (i + distance) % n) for i in range(n)]
    else:
        route = [(i, i + distance) for i in range(n) if 0 <= i + distance < n]
    return lax.ppermute(value, axis, route)


def gather_pieces(own, first, second):
    ahead, behind, across = shift(own, first, -1), shift(own, first, 1), shift(own, first, 2)
    low = jnp.stack([own, ahead])
    high = jnp.stack([across, behind])
    low_ahead, low_behind = shift(low, second, -1), shift(low, second, 1)
    high_ahead, high_behind = shift(high, second, -1), shift(high, second, 1)
    low_across = shift(low_behind, second, 1)
    high_across = shift(high_ahead, second, -1)
    mine = (low, high, low_ahead, high_ahead, low_behind, high_behind, low_across, high_across)
    return mine + tuple(shift(p, AC, 1) for p in mine)


PIECES = 16


def placements(first_at, second_at, core):
    rows = []
    for own in (0, 1):
        c = core if own == 0 else 1 - core
        for place, r2 in enumerate((0, 1, 3, 2)):
            for half in (0, 1):
                for at in (0, 1):
                    piece = PIECES // 2 * own + 2 * place + half
                    rows.append((piece, at, (first_at + 2 * half + at) & 3, (second_at + r2) & 3, c))
    return rows


def assemble_kernel(place, *refs):
    ups, downs = refs[:PIECES], refs[PIECES : 2 * PIECES]
    w_up, w_down, x_st, st_st, at_st, gp_st, g_st, gh_st, _, gg_st, sem_up, sem_down = refs[2 * PIECES :]
    x, z, c = place[0], place[1], place[2]
    n_up, n_down = w_up.shape[0] // 32, w_down.shape[0] // 32
    copies = []
    for piece, at, fx, fz, core in placements(x, z, c):
        rows = pl.ds(pl.multiple_of((fx * 8 + fz * 2 + core) * n_up, n_up), n_up)
        copies.append(pltpu.make_async_copy(ups[piece].at[at], w_up.at[rows], sem_up.at[len(copies)]))
    late = []
    for piece, at, fz, fx, core in placements(z, x, c):
        rows = pl.ds(pl.multiple_of((fx * 8 + fz * 2 + core) * n_down, n_down), n_down)
        late.append(pltpu.make_async_copy(downs[piece].at[at], w_down.at[rows], sem_down.at[len(late)]))
    for copy in copies + late:
        copy.start()
    for ref in (st_st, at_st, g_st, gh_st, gg_st):

        @pl.loop(0, ref.shape[0] // 64)
        def clear(i, ref=ref):
            ref[pl.ds(pl.multiple_of(i * 64, 64), 64), :] = jnp.zeros((64, ref.shape[1]), ref.dtype)

    for copy in copies + late:
        copy.wait()


def assemble(place, ups, downs, micros, rows):
    feat, hidden, tokens = 32 * ups[0].shape[1], ups[0].shape[2], micros * rows
    shapes = (
        (feat, hidden),
        (hidden, feat),
        (tokens, feat),
        (feat, tokens),
        (hidden, tokens),
        (tokens, hidden),
        (tokens, feat),
        (tokens, hidden),
        (rows, feat),
    )
    return pl.pallas_call(
        assemble_kernel,
        out_shape=tuple(pltpu.VMEM(s, BF16) for s in shapes) + (pltpu.VMEM((8 * micros, feat), F32),),
        in_specs=[SMEM] + [ANY] * (2 * PIECES),
        out_specs=(VMEM,) * 10,
        scratch_shapes=[pltpu.SemaphoreType.DMA((32,)), pltpu.SemaphoreType.DMA((32,))],
        compiler_params=pltpu.CompilerParams(vmem_limit_bytes=GRANT),
        name="assemble",
    )(place, *ups, *downs)


def norm_of(values, mask, width):
    mean = jnp.sum(values, axis=-1, keepdims=True) / width
    centered = jnp.where(mask, values - mean, 0.0)
    variance = jnp.sum(centered * centered, axis=-1, keepdims=True) / width
    inv_std = lax.rsqrt(variance + EPSILON)
    return centered * inv_std, inv_std


def held(value):
    return pltpu.with_memory_space_constraint(value, pltpu.VMEM)


def cost_of(flops):
    return pl.CostEstimate(flops=flops, transcendentals=0, bytes_accessed=0)


def span(index, size):
    return pl.ds(pl.multiple_of(index * size, size), size)


def job_of(tab, q, micros):
    sec = tab[4 * micros]
    at = jnp.clip(q, 0, micros - 1)
    micro, width, hidden, depth = tab[at], tab[micros + at], tab[2 * micros + at], tab[3 * micros + at]
    valid = jnp.logical_and(jnp.logical_and(q >= 0, q < micros), depth > sec)
    return sec, at, micro, width, hidden, depth, valid


def forward_kernel(tab, patches, incoming, w_up, w_down, _x, _st, _at, _gp, *refs, tick):
    out, x_st, st_st, at_st, gp_st, normed, hid_buf, act_buf, acc = refs
    micros, rows, _ = patches.shape
    sec, at, micro, width, hidden, _, valid = job_of(tab, tick - SKEW * tab[4 * micros], micros)

    @pl.when(valid)
    def run():
        used = (hidden + CHUNK - 1) // CHUNK
        mine = span(at, rows)

        @pl.when(sec == 0)
        def first():
            acc[...] = patches[micro].astype(F32)

        @pl.when(sec != 0)
        def later():
            acc[...] = incoming[...].astype(F32)

        mask = lax.broadcasted_iota(jnp.int32, acc.shape, 1) < width
        values = jnp.where(mask, acc[...], 0.0)
        acc[...] = values
        x_st[mine, :] = values.astype(BF16)
        standard, _ = norm_of(values, mask, width.astype(F32))
        normed[...] = standard.astype(BF16)
        st_st[:, mine] = standard.T.astype(BF16)
        act_buf[...] = jnp.zeros(act_buf.shape, BF16)
        hid_buf[...] = jnp.dot(normed[...], w_up[:, :CHUNK], preferred_element_type=F32)

        @pl.loop(0, used)
        def step(c):
            h, ready = hid_buf[...], act_buf[...]
            following = jnp.minimum(c + 1, used - 1)
            hid_next = jnp.dot(normed[...], w_up[:, span(following, CHUNK)], preferred_element_type=F32)
            before = jnp.maximum(c - 1, 0)
            acc[...] += jnp.dot(ready, w_down[span(before, CHUNK), :], preferred_element_type=F32)
            h2 = h * h
            t = jnp.tanh(h * (GELU_A + GELU_B * h2))
            p = 0.5 + 0.5 * t
            act = h * p
            slope = p + act * (1.0 - t) * (GELU_A + (3.0 * GELU_B) * h2)
            inside = lax.broadcasted_iota(jnp.int32, h.shape, 1) < hidden - c * CHUNK
            act = jnp.where(inside, act, 0.0)
            act_buf[...] = act.astype(BF16)
            at_st[span(c, CHUNK), mine] = act.T.astype(BF16)
            gp_st[mine, span(c, CHUNK)] = jnp.where(inside, slope, 0.0).astype(BF16)
            hid_buf[...] = hid_next

        total = acc[...] + jnp.dot(act_buf[...], w_down[span(used - 1, CHUNK), :], preferred_element_type=F32)
        out[...] = jnp.where(mask, total, 0.0).astype(BF16)


def forward(tick, tab, patches, incoming, w_up, w_down, stash):
    _, rows, feat = patches.shape
    operands = [tab, held(patches), held(incoming), held(w_up), held(w_down)] + [held(s) for s in stash]
    out, *stash = pl.pallas_call(
        functools.partial(forward_kernel, tick=tick),
        out_shape=(jax.ShapeDtypeStruct((rows, feat), BF16),) + tuple(pltpu.VMEM(s.shape, s.dtype) for s in stash),
        in_specs=[SMEM] + [VMEM] * 8,
        out_specs=(VMEM,) * 5,
        scratch_shapes=[
            pltpu.VMEM((rows, feat), BF16),
            pltpu.VMEM((rows, CHUNK), F32),
            pltpu.VMEM((rows, CHUNK), BF16),
            pltpu.VMEM((rows, feat), F32),
        ],
        input_output_aliases={5 + k: 1 + k for k in range(4)},
        compiler_params=pltpu.CompilerParams(vmem_limit_bytes=TICK_GRANT),
        cost_estimate=cost_of(4 * rows * feat * w_up.shape[1]),
        name="forward",
    )(*operands)
    return out, tuple(stash)


def backward_kernel(tab, cotangent, incoming, w_up, w_down, x_st, gp_st, _at, _g, _gh, _gg, *refs, tick):
    out, g_st, gh_st, gg_st, g_buf, gh_buf, acc = refs
    micros, rows, _ = cotangent.shape
    q = (micros - 1) - (tick + SKEW * (tab[4 * micros] - 1))
    sec, at, micro, width, hidden, depth, valid = job_of(tab, q, micros)

    @pl.when(valid)
    def run():
        used = (hidden + CHUNK - 1) // CHUNK
        mine = span(at, rows)

        @pl.when(depth == sec + 1)
        def last():
            g_buf[...] = cotangent[micro]

        @pl.when(depth != sec + 1)
        def inner():
            g_buf[...] = incoming[...]

        mask = lax.broadcasted_iota(jnp.int32, acc.shape, 1) < width
        grad_branch = jnp.where(mask, g_buf[...].astype(F32), 0.0).astype(BF16)
        g_buf[...] = grad_branch
        g_st[mine, :] = grad_branch
        acc[...] = jnp.zeros(acc.shape, F32)
        gh_buf[...] = jnp.zeros(gh_buf.shape, BF16)
        nt = (((1,), (1,)), ((), ()))

        @pl.loop(0, used)
        def step(c):
            ready = gh_buf[...]
            grad_act = lax.dot_general(g_buf[...], w_down[span(c, CHUNK), :], nt, preferred_element_type=F32)
            before = jnp.maximum(c - 1, 0)
            acc[...] += lax.dot_general(ready, w_up[:, span(before, CHUNK)], nt, preferred_element_type=F32)
            grad_hid = (grad_act * gp_st[mine, span(c, CHUNK)].astype(F32)).astype(BF16)
            gh_buf[...] = grad_hid
            gh_st[mine, span(c, CHUNK)] = grad_hid

        total = acc[...] + lax.dot_general(
            gh_buf[...], w_up[:, span(used - 1, CHUNK)], nt, preferred_element_type=F32
        )
        width_float = width.astype(F32)
        standard, inv_std = norm_of(x_st[mine, :].astype(F32), mask, width_float)
        grad_std = jnp.where(mask, total, 0.0)
        product = grad_std * standard
        gg_st[span(at, 8), :] = jnp.sum(product.reshape(-1, 8, product.shape[1]), axis=0)
        first_mean = jnp.sum(grad_std, axis=-1, keepdims=True) / width_float
        second_mean = jnp.sum(product, axis=-1, keepdims=True) / width_float
        grad_in = inv_std * (grad_std - first_mean - standard * second_mean)
        out[...] = jnp.where(mask, g_buf[...].astype(F32) + grad_in, 0.0).astype(BF16)


def backward(tick, tab, cotangent, incoming, w_up, w_down, x_st, gp_st, at_st, stash):
    _, rows, feat = cotangent.shape
    operands = [tab] + [held(v) for v in (cotangent, incoming, w_up, w_down, x_st, gp_st, at_st) + tuple(stash)]
    out, *stash = pl.pallas_call(
        functools.partial(backward_kernel, tick=tick),
        out_shape=(jax.ShapeDtypeStruct((rows, feat), BF16),) + tuple(pltpu.VMEM(s.shape, s.dtype) for s in stash),
        in_specs=[SMEM] + [VMEM] * 10,
        out_specs=(VMEM,) * 4,
        scratch_shapes=[
            pltpu.VMEM((rows, feat), BF16),
            pltpu.VMEM((rows, CHUNK), BF16),
            pltpu.VMEM((rows, feat), F32),
        ],
        input_output_aliases={8 + k: 1 + k for k in range(3)},
        compiler_params=pltpu.CompilerParams(vmem_limit_bytes=TICK_GRANT),
        cost_estimate=cost_of(4 * rows * feat * w_up.shape[1]),
        name="backward",
    )(*operands)
    return out, tuple(stash)


def split_cores(core, blocks, mine, theirs, value_of):
    for parity, targets in ((0, (mine, theirs)), (1, (theirs, mine))):

        @pl.when(core == parity)
        def write(targets=targets):
            for f in range(blocks):
                targets[f & 1](f >> 3, (f >> 1) & 3, value_of(f))


def up_kernel(place, st, gh, gg, own, par, *, start, with_gain):
    x, z, core = place[0], place[1], place[2]
    width = own.shape[3] - (128 if with_gain else 0)
    n = st.shape[0] // 32

    def put(ref, columns):
        def write(fx, fz, value):
            ref[(fx - x) & 3, (fz - z) & 3, :, columns] = value

        return write

    @pl.loop(0, width // GRAD_CHUNK)
    def step(c):
        columns = span(c, GRAD_CHUNK)
        up = jnp.dot(st[...], gh[:, span(c + start // GRAD_CHUNK, GRAD_CHUNK)], preferred_element_type=F32).astype(BF16)
        split_cores(core, 32, put(own, columns), put(par, columns), lambda f: up[f * n : (f + 1) * n])

    if with_gain:
        total = gg[...]
        total = jnp.concatenate([total, jnp.zeros((128 - total.shape[0], total.shape[1]), F32)], axis=0)
        column = total.T.astype(BF16)
        last = pl.ds(width, 128)
        split_cores(core, 32, put(own, last), put(par, last), lambda f: column[f * n : (f + 1) * n])


def up_grads(place, st_st, gh_st, gg_st, start, width, with_gain):
    feat = st_st.shape[0]
    out = jax.ShapeDtypeStruct((4, 4, feat // 32, width + (128 if with_gain else 0)), BF16)
    return pl.pallas_call(
        functools.partial(up_kernel, start=start, with_gain=with_gain),
        out_shape=(out, out),
        in_specs=[SMEM] + [VMEM] * 3,
        out_specs=(VMEM, VMEM),
        compiler_params=pltpu.CompilerParams(vmem_limit_bytes=GRANT),
        cost_estimate=cost_of(2 * feat * width * gh_st.shape[0]),
        name="up_grads",
    )(place, held(st_st), held(gh_st), held(gg_st))


def down_kernel(place, at, g, own, par):
    x, z, core = place[0], place[1], place[2]
    n = at.shape[0] // 32

    @pl.loop(0, 4)
    def step(i):
        down = jnp.dot(at[span(i, 8 * n), :], g[...], preferred_element_type=F32).astype(BF16)
        for parity, targets in ((0, (own, par)), (1, (par, own))):

            @pl.when(core == parity)
            def write(targets=targets):
                for f in range(8):
                    targets[f & 1][((f >> 1) - z) & 3, (i - x) & 3] = down[f * n : (f + 1) * n]


def down_grads(place, at_st, g_st):
    out = jax.ShapeDtypeStruct((4, 4, at_st.shape[0] // 32, g_st.shape[1]), BF16)
    return pl.pallas_call(
        down_kernel,
        out_shape=(out, out),
        in_specs=[SMEM] + [VMEM] * 2,
        out_specs=(VMEM, VMEM),
        compiler_params=pltpu.CompilerParams(vmem_limit_bytes=GRANT),
        cost_estimate=cost_of(2 * g_st.shape[1] * at_st.shape[0] * at_st.shape[1]),
        name="down_grads",
    )(place, held(at_st), held(g_st))


def plus(*values):
    total = values[0].astype(F32)
    for v in values[1:]:
        total = total + v.astype(F32)
    return total


def scatter_sum(parts, first, second):
    pairs = [(own, shift(partner, AC, 1)) for own, partner in parts]

    def joined(*at):
        return jnp.concatenate([plus(own[at], other[at]) for own, other in pairs], axis=-1)

    low = shift(joined(2, slice(0, 2)).astype(BF16), first, 1)
    high = shift(joined(2, slice(2, 4)).astype(BF16), first, -1)
    ahead = jnp.concatenate([plus(joined(1, slice(0, 2)), low), joined(1, slice(2, 4))]).astype(BF16)
    behind = jnp.concatenate([joined(3, slice(0, 2)), plus(joined(3, slice(2, 4)), high)]).astype(BF16)
    line = plus(joined(0), shift(ahead, first, 1), shift(behind, first, -1))
    parts = [shift(line[r].astype(BF16), second, r) for r in (1, 2, 3)]
    return plus(line[0], *parts)


def schedule_table(embed_blocks, ratio_index, depth):
    micros = depth.shape[0]
    index = lax.iota(jnp.int32, micros)
    before = jnp.logical_or(
        depth[None, :] > depth[:, None],
        jnp.logical_and(depth[None, :] == depth[:, None], index[None, :] < index[:, None]),
    )
    rank = jnp.sum(before.astype(jnp.int32), axis=1)
    chosen = rank[None, :] == index[:, None]
    width = embed_blocks * BLOCK
    hidden = width * (6 + ratio_index) // 2
    columns = jnp.stack([index, width, hidden, depth])
    table = jnp.sum(jnp.where(chosen[None], columns[:, None, :], 0), axis=2)
    section = lax.axis_index("section").astype(jnp.int32)
    return jnp.concatenate([table.reshape(-1), jnp.full((8,), section, jnp.int32)])


def window(extra, tab, place, gain, patches, cotangent, ups, downs):
    micros, rows, _ = patches.shape
    up, down, *stash, g_st, gh_st, unread, gg_st = assemble(place, ups, downs, micros, rows)
    hidden = up.shape[1]
    main = micros + SKEW

    outs = []
    for t in range(main + extra):
        incoming = shift(outs[t - SKEW], "section", 1, wrap=False) if t >= SKEW else unread
        out, stash = forward(t, tab, patches, incoming, up, down, stash)
        outs.append(out)
    x_st, st_st, at_st, gp_st = stash

    back = (g_st, gh_st, gg_st)
    outs = []
    for t in range(main + extra):
        incoming = shift(outs[t - SKEW], "section", -1, wrap=False) if t >= SKEW else unread
        out, back = backward(t - extra, tab, cotangent, incoming, up, down, x_st, gp_st, at_st, back)
        outs.append(out)
    g_st, gh_st, gg_st = back

    down_own, down_par = down_grads(place, at_st, g_st)
    half = hidden // 2
    up_parts = [up_grads(place, st_st, gh_st, gg_st, k * half, half, k == 1) for k in range(2)]
    down_sum = scatter_sum([(down_own, down_par)], AZ, AX)
    up_sum = scatter_sum(up_parts, AX, AZ)
    grad_up = up_sum[:, :hidden] * gain
    grad_gain = jnp.sum(up_sum[:, hidden:], axis=1) / gain[:, 0]
    return grad_up, down_sum, grad_gain


def per_device(patches, cotangent, embed_blocks, ratio_index, depth, w_up, w_down, ln_gain):
    sections = lax.axis_size("section")
    micros = patches.shape[0]
    gain = ln_gain[0].astype(F32)[:, None]
    place = jnp.stack([lax.axis_index(a) for a in FSDP]).astype(jnp.int32)
    tab = schedule_table(embed_blocks, ratio_index, depth)
    scaled = (w_up[0].astype(F32) * gain).astype(BF16)
    ups = gather_pieces(scaled, AX, AZ)
    downs = gather_pieces(w_down[0], AZ, AX)

    extra = jnp.zeros((), jnp.int32)
    for s in range(2, sections):
        reach = jnp.sum((depth > s).astype(jnp.int32))
        extra = jnp.maximum(extra, reach - (micros - SKEW * (s - 1)))
    choices = (0, 1, SKEW * (sections - 2))
    branch = (extra > choices[0]).astype(jnp.int32) + (extra > choices[1]).astype(jnp.int32)
    results = lax.switch(
        branch,
        [functools.partial(window, n) for n in choices],
        *(tab, place, gain, patches, cotangent, ups, downs),
    )
    return tuple(r[None] for r in results)


def solution(mesh):
    finer = Mesh(
        mesh.devices.reshape(mesh.shape["section"], 4, 4, 2),
        ("section",) + FSDP,
    )
    in_specs = (
        P(None, FSDP, None),
        P(None, FSDP, None),
        P(),
        P(),
        P(),
        P("section", FSDP, None),
        P("section", FSDP, None),
        P("section", FSDP),
    )
    out_specs = (P("section", FSDP, None), P("section", FSDP, None), P("section", FSDP))
    return jax.shard_map(
        per_device, mesh=finer, in_specs=in_specs, out_specs=out_specs, check_vma=False
    )
```
